128 devices in a mesh: ep: 32 (over y, x, core), tp: 4 (over z).
Axes of the slice: x: 4, y: 4, z: 4, core: 2. Of those that a mesh axis runs over, the one named last changes fastest.
Arguments:
- tokens: bfloat16 [8192, 7168], P('ep', 'tp'), may hold values from -78 to 78
- norm_gain: bfloat16 [7168], P('tp'), may hold values from 0.5 to 1.5
- expert_ids: int32 [8192, 8], P('ep'), may hold values from 0 to 255, all different within a row
- gate_prob: bfloat16 [8192, 8], P('ep'), may hold values from 0.049804688 to 1
- w_gate: bfloat16 [32, 7168, 2048], P('ep', None, 'tp'), may hold values from -0.0625 to 0.0625
- w_up: bfloat16 [32, 7168, 2048], P('ep', None, 'tp'), may hold values from -0.0625 to 0.0625
- w_down: bfloat16 [32, 2048, 7168], P('ep', 'tp'), may hold values from -0.125 to 0.125
Outputs:
- combined: bfloat16 [8192, 7168], P('ep', 'tp')
The draws below stay inside these ranges and needn't reach their ends.
Inputs may be any that keep to these rules, and one draw needn't show every extreme that they name: `expert_ids`: each row names 8 different experts.
All inputs are finite; a program needn't handle non-finite values.
Results may differ from the reference program's by a relative error of at most 0.01.
Values may be sent and summed in bfloat16 or wider, within the bound.
A program may use at most 128 MiB of HBM per device.

```python
import math
import jax
import jax.numpy as jnp
from jax import lax

D = 7168
FF = 2048
TOP = 8
TOK_DEV = 256
EXPERTS = 256
WINDOW = 32
TOKENS = 8192
CAP = 16
N_TP = 4


def draw_tokens(key, part):
    base_key = jax.random.fold_in(key, 11)
    row_key = jax.random.fold_in(key, 12)
    col_key = jax.random.fold_in(key, 13)
    rows_scale = jnp.exp(jax.random.uniform(row_key, (TOKENS, 1), jnp.float32, math.log(0.3), math.log(3.0)))
    rising = 3.0 ** (jnp.arange(D, dtype=jnp.float32) / D - 0.5)
    cols_scale = rising * jnp.exp(jax.random.uniform(col_key, (D,), jnp.float32, math.log(0.4), math.log(2.5)))
    base = jnp.clip(jax.random.normal(base_key, (TOKENS, D), jnp.float32), -6.0, 6.0)
    return (base * rows_scale * cols_scale[None, :]).astype(jnp.bfloat16)


def block_levels(key, shape, pieces, low, largest):
    def one(dim, shards_of):
        heights = jax.random.uniform(jax.random.fold_in(jax.random.fold_in(key, 6), dim), (shards_of,), jnp.float32, low / len(pieces), largest / len(pieces))
        return jnp.repeat(jnp.exp(heights), shape[dim] // shards_of).reshape((-1,) + (1,) * (len(shape) - dim - 1))

    factor_of = one(*pieces[0])
    for cut in pieces[1:]:
        factor_of = factor_of * one(*cut)
    return factor_of


def distinct(own_key, rows, amount, top, lift):
    sequence = jax.random.permutation(jax.random.fold_in(own_key, 1), amount)
    boost = sequence
    for power in range(3):
        boost = boost * boost // amount
    boost = boost * lift // amount
    lots = jax.random.randint(jax.random.fold_in(own_key, 2), (rows, amount), 0, 4096) + boost
    sure = jax.random.permutation(jax.random.fold_in(own_key, 3), rows)[jnp.arange(amount) % rows]
    lots = jnp.where(jnp.arange(rows)[:, None] == sure[None, :], 1 << 14, lots)
    score = lots * amount + jnp.arange(amount)
    return lax.top_k(score.astype(jnp.int32), top)[1].astype(jnp.int32)


def noise(own_key, shape, width, reach, shards=(), kind=jnp.bfloat16):
    array = jax.random.normal(own_key, shape, jnp.float32) * width
    if len(shards) > 0:
        array = block_levels(own_key, shape, shards, -0.22, 0.18) * array
    return jnp.clip(array, min=-reach, max=reach).astype(kind)


def setup_inputs(seed: int = 0) -> dict:
    arg_keys = jax.random.split(jax.random.key(seed), 8)
    tokens = draw_tokens(jax.random.fold_in(arg_keys[7], 71), 0)
    norm_gain = jnp.clip(1.0 + 0.1 * jax.random.normal(arg_keys[1], (D,), jnp.float32), 0.5, 1.5).astype(jnp.bfloat16)
    expert_ids = distinct(arg_keys[2], TOKENS, EXPERTS, TOP, 512)
    gate_prob = jnp.clip(jnp.exp(math.log(1.0) - 2.9996462 * jax.random.uniform(arg_keys[3], (TOKENS, TOP), jnp.float32) ** block_levels(arg_keys[3], (TOKENS, TOP), ((0, 32),), -0.2, 0.2)), 0.049804688, 1.0).astype(jnp.bfloat16)
    w_gate = noise(arg_keys[4], (WINDOW, D, FF), D ** -0.5, 0.0625, ((0, 32), (2, 4)))
    w_up = noise(arg_keys[5], (WINDOW, D, FF), D ** -0.5, 0.0625, ((0, 32), (2, 4)))
    w_down = noise(arg_keys[6], (WINDOW, FF, D), FF ** -0.5, 0.125, ((0, 32), (1, 4)))
    return dict(tokens=tokens, norm_gain=norm_gain, expert_ids=expert_ids, gate_prob=gate_prob, w_gate=w_gate, w_up=w_up, w_down=w_down)


epsilon = 1e-06

def slots_of(expert_ids):
    is_live = expert_ids < WINDOW
    matches = (expert_ids[:, :, None] == jnp.arange(WINDOW, dtype=jnp.int32)).astype(jnp.int32)
    counts = lax.optimization_barrier(jnp.sum(matches, axis=1))
    blocked = counts.reshape(-1, TOK_DEV, WINDOW)
    before = (jnp.cumsum(blocked, axis=1) - blocked).reshape(-1, WINDOW)
    slot_index = lax.optimization_barrier(jnp.sum(matches * before[:, None, :], axis=2))
    is_kept = is_live & (slot_index < CAP)
    return (slot_index, is_kept)

def reference(tokens, norm_gain, expert_ids, gate_prob, w_gate, w_up, w_down):
    values = tokens.astype(jnp.float32)
    mean_square = lax.optimization_barrier(jnp.mean(values * values, axis=1, keepdims=True))
    normed = (values * lax.rsqrt(mean_square + epsilon) * norm_gain.astype(jnp.float32)).astype(jnp.bfloat16)
    slot_index, is_kept = slots_of(expert_ids)
    block_count = TOKENS // TOK_DEV
    block_index = (jnp.arange(TOKENS, dtype=jnp.int32) // TOK_DEV)[:, None]
    slot_total = WINDOW * block_count * CAP
    flat_index = jnp.where(is_kept, (expert_ids * block_count + block_index) * CAP + slot_index, slot_total).astype(jnp.int32)
    buffer = jnp.zeros((slot_total, D), jnp.bfloat16)
    for column in range(TOP):
        buffer = buffer.at[flat_index[:, column]].set(normed, mode='drop')
    buffer = buffer.reshape(WINDOW, block_count * CAP, D)
    block_width = FF // N_TP

    def one_expert(operands):
        rows_in, gate_matrix, up_matrix, down_matrix = operands
        gate_act = jnp.dot(rows_in, gate_matrix, preferred_element_type=jnp.float32)
        up_act = jnp.dot(rows_in, up_matrix, preferred_element_type=jnp.float32)
        hidden = (jax.nn.silu(gate_act) * up_act).astype(jnp.bfloat16)
        summed = jnp.zeros((rows_in.shape[0], D), jnp.float32)
        for block_number in range(N_TP):
            lower = block_number * block_width
            down_part = jnp.dot(hidden[:, lower:lower + block_width], down_matrix[lower:lower + block_width], preferred_element_type=jnp.float32)
            rounded = lax.optimization_barrier(down_part.astype(jnp.bfloat16))
            summed = summed + rounded.astype(jnp.float32)
        return summed.astype(jnp.bfloat16)
    expert_out = lax.map(one_expert, (buffer, w_gate, w_up, w_down)).reshape(slot_total, D)
    combined = jnp.zeros((TOKENS, D), jnp.float32)
    for column in range(TOP):
        picked = jnp.take(expert_out, flat_index[:, column], axis=0, mode='fill', fill_value=0).astype(jnp.float32)
        combined = combined + gate_prob[:, column:column + 1].astype(jnp.float32) * picked
    return combined.astype(jnp.bfloat16)
```

```python
import functools

import jax
import jax.numpy as jnp
from jax import lax
from jax.experimental import pallas as pl
from jax.experimental.pallas import tpu as pltpu
from jax.sharding import PartitionSpec as P

MESH = pl.DeviceIdType.MESH
F32 = jnp.float32
BF16 = jnp.bfloat16

D = 7168
CAP = 16
CORES = 2
NZ = 4
CHUNK = 256
ROUTE_A = 4
WEIGHT_PIECES = 4
epsilon = 1e-06


def moe_kernel(
    cfg,
    tokens_ref,
    gain_ref,
    ids_ref,
    prob_ref,
    wg_hbm,
    wu_hbm,
    wd_hbm,
    out_ref,
    wg,
    wu,
    wd,
    sq_buf,
    disp_t,
    comb,
    xa,
    xb,
    nb,
    out_a,
    out_b,
    acc_g,
    acc_u,
    hid,
    far_a,
    far_in_a,
    near_a,
    near_in_a,
    ret_a,
    ret_b,
    far_b,
    far_in_b,
    near_b,
    near_in_b,
    w_sem,
    sq_send,
    sq_recv,
    da_send,
    da_recv,
    db_send,
    db_recv,
    za_send,
    za_recv,
    zb_send,
    zb_recv,
    ra_send,
    ra_recv,
    rb_send,
    rb_recv,
    ya_send,
    ya_recv,
    yb_send,
    yb_recv,
):
    E, NA, NB, CW, FFD = cfg["E"], cfg["NA"], cfg["NB"], cfg["CW"], cfg["FFD"]
    DZ, T = cfg["DZ"], cfg["T"]
    S = E * CAP
    EH = E // 2
    SH = S // 2
    TH = T // 2
    e = lax.axis_index("ep")
    z = lax.axis_index("tp")
    zp = lax.rem(z + 1, NZ)
    zm = lax.rem(z + 3, NZ)
    zf = lax.rem(z + 2, NZ)

    def peer_of(k):
        off = lax.rem(k * cfg["STRIDE"], E)
        chip = lax.rem(e // CORES + off // CORES, E // CORES)
        if cfg["NX"] > 1:
            nx = cfg["NX"]
            oc = off // CORES
            mc = e // CORES
            py = lax.rem(mc // nx + oc // nx, E // CORES // nx)
            px = lax.rem(lax.rem(mc, nx) + lax.rem(oc, nx), nx)
            chip = py * nx + px
        core = lax.rem(lax.rem(e, CORES) + lax.rem(off, CORES), CORES)
        return chip * CORES + core

    def to_z(src, dst, send, recv, zt):
        return pltpu.make_async_remote_copy(
            src_ref=src, dst_ref=dst, send_sem=send, recv_sem=recv, device_id=(e, zt), device_id_type=MESH
        )

    def to_e(src, dst, send, recv, et):
        return pltpu.make_async_remote_copy(
            src_ref=src, dst_ref=dst, send_sem=send, recv_sem=recv, device_id=(et, z), device_id_type=MESH
        )

    def take(ref, sem):
        pltpu.make_async_copy(ref, ref, sem).wait()

    rows_w = wg.shape[0] // WEIGHT_PIECES
    rows_d = wd.shape[0] // WEIGHT_PIECES
    weight_copies = []
    for p in range(WEIGHT_PIECES):
        rs = pl.ds(p * rows_w, rows_w)
        weight_copies.append(pltpu.make_async_copy(wg_hbm.at[rs], wg.at[rs], w_sem.at[0, p]))
        weight_copies.append(pltpu.make_async_copy(wu_hbm.at[rs], wu.at[rs], w_sem.at[1, p]))
    down_copies = []
    for p in range(WEIGHT_PIECES):
        rs = pl.ds(p * rows_d, rows_d)
        down_copies.append(pltpu.make_async_copy(wd_hbm.at[rs], wd.at[rs], w_sem.at[2, p]))

    barrier = pltpu.get_barrier_semaphore()

    def greet(k, carry):
        pl.semaphore_signal(barrier, inc=1, device_id=(peer_of(k), z), device_id_type=MESH)
        return carry

    lax.fori_loop(1, E, greet, 0)
    for dz in range(1, NZ):
        pl.semaphore_signal(barrier, inc=1, device_id=(e, lax.rem(z + dz, NZ)), device_id_type=MESH)
    for copy in weight_copies + down_copies:
        copy.start()

    values = tokens_ref[...].astype(F32)
    part = jnp.sum(values * values, axis=1, keepdims=True)
    if T < 128:
        part = jnp.concatenate([part, jnp.zeros((128 - T, 1), F32)], axis=0)
    TP = max(T, 128)
    part_t = jnp.transpose(jnp.broadcast_to(part, (TP, 128)))
    sq_buf[z] = part_t[0:8, :]
    pl.semaphore_wait(barrier, E - 1 + NZ - 1)
    sq_copies = []
    for dz in range(1, NZ):
        copy = to_z(sq_buf.at[z], sq_buf.at[z], sq_send.at[dz - 1], sq_recv.at[dz - 1], lax.rem(z + dz, NZ))
        copy.start()
        sq_copies.append(copy)

    ids = ids_ref[...]
    probs = prob_ref[...].astype(F32)
    expert_iota = lax.broadcasted_iota(jnp.int32, (T, E), 1)
    match = jnp.zeros((T, E), F32)
    weight = jnp.zeros((T, E), F32)
    for k in range(ids.shape[1]):
        hit = ids[:, k : k + 1] == expert_iota
        match = match + jnp.where(hit, 1.0, 0.0)
        weight = weight + jnp.where(hit, probs[:, k : k + 1], 0.0)
    lower = jnp.where(
        lax.broadcasted_iota(jnp.int32, (T, T), 0) > lax.broadcasted_iota(jnp.int32, (T, T), 1), 1.0, 0.0
    ).astype(BF16)
    match_b = match.astype(BF16)
    before = jnp.dot(lower, match_b, preferred_element_type=F32).astype(BF16)
    spread_row = lax.broadcasted_iota(jnp.int32, (E, S), 0)
    spread_col = lax.broadcasted_iota(jnp.int32, (E, S), 1)
    spread = jnp.where(spread_col // CAP == spread_row, 1.0, 0.0).astype(BF16)
    match_s = jnp.dot(match_b, spread, preferred_element_type=F32)
    before_s = jnp.dot(before, spread, preferred_element_type=F32)
    weight_s = jnp.dot(weight.astype(BF16), spread, preferred_element_type=F32)
    slot_of = lax.rem(lax.broadcasted_iota(jnp.int32, (T, S), 1), CAP).astype(F32)
    chosen = jnp.where((match_s > 0.5) & (before_s == slot_of), 1.0, 0.0)
    comb[...] = (chosen * weight_s).astype(BF16)
    disp_t[...] = jnp.transpose(chosen).astype(BF16)
    acc_g[...] = jnp.zeros_like(acc_g)
    acc_u[...] = jnp.zeros_like(acc_u)

    for copy in sq_copies:
        copy.wait()
    total_t = sq_buf[0] + sq_buf[1] + sq_buf[2] + sq_buf[3]
    total = jnp.transpose(jnp.broadcast_to(total_t[0:1, :], (128, TP)))[0:T, 0:1]
    inverse = lax.rsqrt(total / cfg["D"] + epsilon)

    def cols(c):
        return pl.ds(pl.multiple_of(c * CW, CW), CW)

    def normed(c):
        v = tokens_ref[:, cols(c)].astype(F32)
        return (v * inverse * gain_ref[:, cols(c)].astype(F32)).astype(BF16)

    for c in range(NB):
        nb[c, z] = normed(NA + c)
        for i, zt in ((0, zp), (1, zm)):
            to_z(nb.at[c, z], nb.at[c, z], zb_send.at[i, c], zb_recv.at[i, c], zt).start()

    for c in range(NA):
        rows = jnp.dot(disp_t[...], normed(c), preferred_element_type=F32).astype(BF16)
        out_a[c] = rows.reshape(E, CAP, CW)
        xa[c, z, e] = out_a[c, e]

        def send_a(k, carry, c=c):
            et = peer_of(k)
            to_e(out_a.at[c, et], xa.at[c, z, e], da_send.at[c], da_recv.at[c], et).start()
            return carry

        lax.fori_loop(1, E, send_a, 0)

    def forward_b(c):
        take(nb.at[c, zm], zb_recv.at[0, c])
        lo, hi = pl.ds(0, TH), pl.ds(TH, TH)
        to_z(nb.at[c, zm, lo], nb.at[c, zm, lo], zb_send.at[2, c], zb_recv.at[2, c], zp).start()
        take(nb.at[c, zp], zb_recv.at[1, c])
        to_z(nb.at[c, zp, hi], nb.at[c, zp, hi], zb_send.at[3, c], zb_recv.at[3, c], zm).start()

    def dispatch_b(c):
        take(nb.at[c, zf, pl.ds(0, TH)], zb_recv.at[2, c])
        take(nb.at[c, zf, pl.ds(TH, TH)], zb_recv.at[3, c])
        for q in range(NZ):
            rows = jnp.dot(disp_t[...], nb[c, q], preferred_element_type=F32).astype(BF16)
            out_b[c, :, q] = rows.reshape(E, CAP, CW)
        xb[c, e] = out_b[c, e]

        def send_b(k, carry):
            et = peer_of(k)
            to_e(out_b.at[c, et], xb.at[c, e], db_send.at[c], db_recv.at[c], et).start()
            return carry

        lax.fori_loop(1, E, send_b, 0)

    def direct_a(c):
        take(xa.at[c, z, pl.ds(0, E - 1)], da_recv.at[c])
        for i, zt in ((0, zp), (1, zm)):
            to_z(xa.at[c, z], xa.at[c, z], za_send.at[i, c], za_recv.at[i, c], zt).start()

    def forward_a(c):
        lo, hi = pl.ds(0, EH), pl.ds(EH, EH)
        take(xa.at[c, zm], za_recv.at[0, c])
        to_z(xa.at[c, zm, lo], xa.at[c, zm, lo], za_send.at[2, c], za_recv.at[2, c], zp).start()
        take(xa.at[c, zp], za_recv.at[1, c])
        to_z(xa.at[c, zp, hi], xa.at[c, zp, hi], za_send.at[3, c], za_recv.at[3, c], zm).start()

    def multiply(blocks, base):
        x = jnp.concatenate([b.reshape(S, CW) for b in blocks], axis=1)
        for w_ref, acc in ((wg, acc_g), (wu, acc_u)):
            w = jnp.concatenate(
                [w_ref[pl.ds(pl.multiple_of(q * DZ + base, CW), CW), :] for q in range(NZ)], axis=0
            )
            acc[...] += jnp.dot(x, w, preferred_element_type=F32)

    def matmul_a(c):
        take(xa.at[c, zf, pl.ds(0, EH)], za_recv.at[2, c])
        take(xa.at[c, zf, pl.ds(EH, EH)], za_recv.at[3, c])
        multiply([xa[c, q] for q in range(NZ)], c * CW)

    def matmul_b(c):
        take(xb.at[c, pl.ds(0, E - 1)], db_recv.at[c])
        multiply([xb[c, :, q] for q in range(NZ)], (NA + c) * CW)

    def wait_weights():
        for copy in weight_copies:
            copy.wait()

    def run(steps, count):
        def body(it, carry):
            for fn, first, n in steps:
                if n > 0:

                    @pl.when((it >= first) & (it < first + n))
                    def _(fn=fn, first=first):
                        fn(it - first)

            return carry

        lax.fori_loop(0, count, body, 0)

    wait_weights()
    run(
        (
            (forward_b, 0, NB),
            (direct_a, 0, NA),
            (dispatch_b, 1, NB),
            (forward_a, 1, NA),
            (matmul_a, 2, NA),
            (matmul_b, NB + 1, NB),
        ),
        max(NA + 2, 2 * NB + 1),
    )

    g = acc_g[...]
    hid[...] = (g / (1.0 + jnp.exp(-g)) * acc_u[...]).astype(BF16)
    for copy in down_copies:
        copy.wait()

    def down(q, c):
        ds = pl.ds(pl.multiple_of(q * DZ + c * CW, CW), CW)
        return jnp.dot(hid[...], wd[:, ds], preferred_element_type=F32).astype(BF16)

    lo_s, hi_s = pl.ds(0, SH), pl.ds(SH, SH)

    def far_part_a(c):
        far_a[c] = down(zf, c)
        to_z(far_a.at[c, lo_s], far_in_a.at[c, lo_s], ra_send.at[0, c], ra_recv.at[0, c], zp).start()
        to_z(far_a.at[c, hi_s], far_in_a.at[c, hi_s], ra_send.at[1, c], ra_recv.at[1, c], zm).start()

    def plus(a, b):
        return (a.astype(F32) + b.astype(F32)).astype(BF16)

    def near_part_a(c):
        near_a[c, 0] = down(zp, c)
        near_a[c, 1] = down(zm, c)
        take(far_in_a.at[c, lo_s], ra_recv.at[0, c])
        near_a[c, 0, lo_s] = plus(near_a[c, 0, lo_s], far_in_a[c, lo_s])
        to_z(near_a.at[c, 0], near_in_a.at[c, 0], ra_send.at[2, c], ra_recv.at[2, c], zp).start()
        take(far_in_a.at[c, hi_s], ra_recv.at[1, c])
        near_a[c, 1, hi_s] = plus(near_a[c, 1, hi_s], far_in_a[c, hi_s])
        to_z(near_a.at[c, 1], near_in_a.at[c, 1], ra_send.at[3, c], ra_recv.at[3, c], zm).start()

    def own_part_a(c):
        own = jnp.dot(
            hid[...], wd[:, pl.ds(pl.multiple_of(z * DZ + c * CW, CW), CW)], preferred_element_type=F32
        )
        own = own.astype(BF16).astype(F32)
        take(near_in_a.at[c, 0], ra_recv.at[2, c])
        take(near_in_a.at[c, 1], ra_recv.at[3, c])
        own = own + near_in_a[c, 0].astype(F32) + near_in_a[c, 1].astype(F32)
        out_a[c] = own.astype(BF16).reshape(E, CAP, CW)
        ret_a[c, e] = out_a[c, e]

        def send_back(k, carry):
            et = peer_of(k)
            to_e(out_a.at[c, et], ret_a.at[c, e], ya_send.at[c], ya_recv.at[c], et).start()
            return carry

        lax.fori_loop(1, E, send_back, 0)

    def part_b(c):
        for q in range(NZ):
            out_b[c, :, q] = down(q, NA + c).reshape(E, CAP, CW)
        ret_b[c, e] = out_b[c, e]

        def send_back(k, carry):
            et = peer_of(k)
            to_e(out_b.at[c, et], ret_b.at[c, e], yb_send.at[c], yb_recv.at[c], et).start()
            return carry

        lax.fori_loop(1, E, send_back, 0)

    def weigh_b(c, q):
        return jnp.dot(comb[...], ret_b[c, :, q].reshape(S, CW), preferred_element_type=F32).astype(BF16)

    lo_t, hi_t = pl.ds(0, TH), pl.ds(TH, TH)

    def far_part_b(c):
        take(ret_b.at[c, pl.ds(0, E - 1)], yb_recv.at[c])
        far_b[c] = weigh_b(c, zf)
        to_z(far_b.at[c, lo_t], far_in_b.at[c, lo_t], rb_send.at[0, c], rb_recv.at[0, c], zp).start()
        to_z(far_b.at[c, hi_t], far_in_b.at[c, hi_t], rb_send.at[1, c], rb_recv.at[1, c], zm).start()

    def near_part_b(c):
        near_b[c, 0] = weigh_b(c, zp)
        near_b[c, 1] = weigh_b(c, zm)
        take(far_in_b.at[c, lo_t], rb_recv.at[0, c])
        near_b[c, 0, lo_t] = plus(near_b[c, 0, lo_t], far_in_b[c, lo_t])
        to_z(near_b.at[c, 0], near_in_b.at[c, 0], rb_send.at[2, c], rb_recv.at[2, c], zp).start()
        take(far_in_b.at[c, hi_t], rb_recv.at[1, c])
        near_b[c, 1, hi_t] = plus(near_b[c, 1, hi_t], far_in_b[c, hi_t])
        to_z(near_b.at[c, 1], near_in_b.at[c, 1], rb_send.at[3, c], rb_recv.at[3, c], zm).start()

    def own_part_b(c):
        own = jnp.dot(comb[...], ret_b[c, :, z].reshape(S, CW), preferred_element_type=F32)
        take(near_in_b.at[c, 0], rb_recv.at[2, c])
        take(near_in_b.at[c, 1], rb_recv.at[3, c])
        own = own + near_in_b[c, 0].astype(F32) + near_in_b[c, 1].astype(F32)
        out_ref[:, cols(NA + c)] = own.astype(BF16)

    def combine_a(c):
        take(ret_a.at[c, pl.ds(0, E - 1)], ya_recv.at[c])
        got = jnp.dot(comb[...], ret_a[c].reshape(S, CW), preferred_element_type=F32)
        out_ref[:, cols(c)] = got.astype(BF16)

    def left(ref, sem):
        pltpu.make_async_copy(ref, ref, sem).wait()

    for c in range(NA):
        left(out_a.at[c, pl.ds(0, E - 1)], da_send.at[c])
    for c in range(NB):
        left(out_b.at[c, pl.ds(0, E - 1)], db_send.at[c])

    run(
        (
            (far_part_a, 0, NA),
            (part_b, 0, NB),
            (near_part_a, 1, NA),
            (own_part_a, 2, NA),
            (far_part_b, 3, NB),
            (near_part_b, 4, NB),
        ),
        max(NA + 2, NB + 4),
    )
    for c in range(NA):
        combine_a(c)
    for c in range(NB):
        own_part_b(c)

    for c in range(NA):
        for i in range(2):
            left(xa.at[c, 0], za_send.at[i, c])
            left(xa.at[c, 0, pl.ds(0, EH)], za_send.at[2 + i, c])
            left(far_a.at[c, lo_s], ra_send.at[i, c])
            left(near_a.at[c, 0], ra_send.at[2 + i, c])
        left(out_a.at[c, pl.ds(0, E - 1)], ya_send.at[c])
    for c in range(NB):
        for i in range(2):
            left(nb.at[c, 0], zb_send.at[i, c])
            left(nb.at[c, 0, pl.ds(0, TH)], zb_send.at[2 + i, c])
            left(far_b.at[c, lo_t], rb_send.at[i, c])
            left(near_b.at[c, 0], rb_send.at[2 + i, c])
        left(out_b.at[c, pl.ds(0, E - 1)], yb_send.at[c])


def local(cfg, tokens, norm_gain, expert_ids, gate_prob, w_gate, w_up, w_down):
    E, NA, NB, CW, T = cfg["E"], cfg["NA"], cfg["NB"], cfg["CW"], cfg["T"]
    DZ, FFD = cfg["DZ"], cfg["FFD"]
    S = E * CAP
    a, b = max(NA, 1), max(NB, 1)
    vmem = pl.BlockSpec(memory_space=pltpu.VMEM)
    hbm = pl.BlockSpec(memory_space=pl.ANY)
    TP = max(T, 128)
    dma = pltpu.SemaphoreType.DMA
    scratch = [
        pltpu.VMEM((NZ * DZ, FFD), BF16),
        pltpu.VMEM((NZ * DZ, FFD), BF16),
        pltpu.VMEM((FFD, NZ * DZ), BF16),
        pltpu.VMEM((NZ, 8, TP), F32),
        pltpu.VMEM((S, T), BF16),
        pltpu.VMEM((T, S), BF16),
        pltpu.VMEM((a, NZ, E, CAP, CW), BF16),
        pltpu.VMEM((b, E, NZ, CAP, CW), BF16),
        pltpu.VMEM((b, NZ, T, CW), BF16),
        pltpu.VMEM((a, E, CAP, CW), BF16),
        pltpu.VMEM((b, E, NZ, CAP, CW), BF16),
        pltpu.VMEM((S, FFD), F32),
        pltpu.VMEM((S, FFD), F32),
        pltpu.VMEM((S, FFD), BF16),
        pltpu.VMEM((a, S, CW), BF16),
        pltpu.VMEM((a, S, CW), BF16),
        pltpu.VMEM((a, 2, S, CW), BF16),
        pltpu.VMEM((a, 2, S, CW), BF16),
        pltpu.VMEM((a, E, CAP, CW), BF16),
        pltpu.VMEM((b, E, NZ, CAP, CW), BF16),
        pltpu.VMEM((b, T, CW), BF16),
        pltpu.VMEM((b, T, CW), BF16),
        pltpu.VMEM((b, 2, T, CW), BF16),
        pltpu.VMEM((b, 2, T, CW), BF16),
        dma((3, WEIGHT_PIECES)),
        dma((NZ - 1,)),
        dma((NZ - 1,)),
        dma((a,)),
        dma((a,)),
        dma((b,)),
        dma((b,)),
        dma((4, a)),
        dma((4, a)),
        dma((4, b)),
        dma((4, b)),
        dma((4, a)),
        dma((4, a)),
        dma((4, b)),
        dma((4, b)),
        dma((a,)),
        dma((a,)),
        dma((b,)),
        dma((b,)),
    ]
    return pl.pallas_call(
        functools.partial(moe_kernel, cfg),
        out_shape=jax.ShapeDtypeStruct((T, DZ), BF16),
        in_specs=[vmem, vmem, vmem, vmem, hbm, hbm, hbm],
        out_specs=vmem,
        scratch_shapes=scratch,
        compiler_params=pltpu.CompilerParams(
            collective_id=0, has_side_effects=True, vmem_limit_bytes=cfg["VMEM"]
        ),
        name="moe_layer",
    )(tokens, norm_gain.reshape(1, -1), expert_ids, gate_prob, w_gate[0], w_up[0], w_down[0])


def config(mesh, tokens=8192, width=D, ff=2048, chunk=CHUNK, route_a=ROUTE_A, nx=4):
    E = mesh.shape["ep"]
    DZ = width // NZ
    n = DZ // chunk
    return dict(
        E=E,
        T=tokens // E,
        D=width,
        DZ=DZ,
        FFD=ff // NZ,
        CW=chunk,
        NA=route_a,
        NB=n - route_a,
        NX=nx,
        STRIDE=11,
        VMEM=67_000_000,
    )


def build(mesh, cfg):
    placed = (
        P("ep", "tp"),
        P("tp"),
        P("ep", None),
        P("ep", None),
        P("ep", None, "tp"),
        P("ep", None, "tp"),
        P("ep", "tp", None),
    )
    return jax.shard_map(
        functools.partial(local, cfg), mesh=mesh, in_specs=placed, out_specs=P("ep", "tp"), check_vma=False
    )


def solution(mesh):
    return build(mesh, config(mesh))
```

```python
import functools

import jax
import jax.numpy as jnp
from jax import lax
from jax.experimental import pallas as pl
from jax.experimental.pallas import tpu as pltpu
from jax.sharding import PartitionSpec as P

MESH = pl.DeviceIdType.MESH
F32 = jnp.float32
BF16 = jnp.bfloat16

D = 7168
CAP = 16
CORES = 2
NZ = 4
WIDTHS_A = (256, 256, 256, 256)
WIDTHS_B = (256, 256, 256)
WEIGHT_PIECES = 4
epsilon = 1e-06


def moe_kernel(
    cfg,
    tokens_hbm,
    gain_ref,
    ids_ref,
    prob_ref,
    wg_hbm,
    wu_hbm,
    wd_hbm,
    out_ref,
    tokens,
    sc_out,
    sc_in,
    scales,
    wg,
    wu,
    wd,
    sq_buf,
    disp_t,
    comb,
    acc_g,
    acc_u,
    hid,
    t_sem,
    w_sem,
    sc_send,
    sc_recv,
    sq_send,
    sq_recv,
    per_a,
    per_b,
    sem_a,
    sem_b,
):
    xa, out_a, far_a, far_in_a, near_a, near_in_a, ret_a = per_a
    xb, nb, out_b, ret_b, far_b, far_in_b, near_b, near_in_b = per_b
    da_send, da_recv, za_send, za_recv, ra_send, ra_recv, ya_send, ya_recv = sem_a
    db_send, db_recv, zb_send, zb_recv, rb_send, rb_recv, yb_send, yb_recv = sem_b
    E, A, B = cfg["E"], cfg["A"], cfg["B"]
    NA, NB = len(A), len(B)
    DZ, T = cfg["DZ"], cfg["T"]
    S = E * CAP
    EH = E // 2
    SH = S // 2
    TH = T // 2
    e = lax.axis_index("ep")
    z = lax.axis_index("tp")
    zp = lax.rem(z + 1, NZ)
    zm = lax.rem(z + 3, NZ)
    zf = lax.rem(z + 2, NZ)

    def peer_of(k):
        off = lax.rem(k * cfg["STRIDE"], E)
        chip = lax.rem(e // CORES + off // CORES, E // CORES)
        if cfg["NX"] > 1:
            nx = cfg["NX"]
            oc = off // CORES
            mc = e // CORES
            py = lax.rem(mc // nx + oc // nx, E // CORES // nx)
            px = lax.rem(lax.rem(mc, nx) + lax.rem(oc, nx), nx)
            chip = py * nx + px
        core = lax.rem(lax.rem(e, CORES) + lax.rem(off, CORES), CORES)
        return chip * CORES + core

    def to_z(src, dst, send, recv, zt):
        return pltpu.make_async_remote_copy(
            src_ref=src, dst_ref=dst, send_sem=send, recv_sem=recv, device_id=(e, zt), device_id_type=MESH
        )

    def to_e(src, dst, send, recv, et):
        return pltpu.make_async_remote_copy(
            src_ref=src, dst_ref=dst, send_sem=send, recv_sem=recv, device_id=(et, z), device_id_type=MESH
        )

    def take(ref, sem):
        pltpu.make_async_copy(ref, ref, sem).wait()

    barrier = pltpu.get_barrier_semaphore()

    def greet(k, carry):
        pl.semaphore_signal(barrier, inc=1, device_id=(peer_of(k), z), device_id_type=MESH)
        return carry

    for dz in range(1, NZ):
        pl.semaphore_signal(barrier, inc=1, device_id=(e, lax.rem(z + dz, NZ)), device_id_type=MESH)
    lax.fori_loop(1, E, greet, 0)

    token_copy = pltpu.make_async_copy(tokens_hbm, tokens, t_sem)
    token_copy.start()
    rows_w = wg.shape[0] // WEIGHT_PIECES
    rows_d = wd.shape[0] // WEIGHT_PIECES
    weight_copies = []
    for p in range(WEIGHT_PIECES):
        rs = pl.ds(p * rows_w, rows_w)
        weight_copies.append(pltpu.make_async_copy(wg_hbm.at[rs], wg.at[rs], w_sem.at[0, p]))
        weight_copies.append(pltpu.make_async_copy(wu_hbm.at[rs], wu.at[rs], w_sem.at[1, p]))
    down_copies = []
    for p in range(WEIGHT_PIECES):
        rs = pl.ds(p * rows_d, rows_d)
        down_copies.append(pltpu.make_async_copy(wd_hbm.at[rs], wd.at[rs], w_sem.at[2, p]))

    ids = ids_ref[...]
    probs = prob_ref[...].astype(F32)
    expert_iota = lax.broadcasted_iota(jnp.int32, (E, T), 0)
    match = jnp.zeros((E, T), F32)
    weight = jnp.zeros((E, T), F32)
    for k in range(ids.shape[0]):
        hit = ids[k : k + 1, :] == expert_iota
        match = match + jnp.where(hit, 1.0, 0.0)
        weight = weight + jnp.where(hit, probs[k : k + 1, :], 0.0)
    earlier = jnp.where(
        lax.broadcasted_iota(jnp.int32, (T, T), 0) < lax.broadcasted_iota(jnp.int32, (T, T), 1), 1.0, 0.0
    ).astype(BF16)
    match_b = match.astype(BF16)
    before = jnp.dot(match_b, earlier, preferred_element_type=F32).astype(BF16)
    spread = jnp.where(
        lax.broadcasted_iota(jnp.int32, (S, E), 0) // CAP == lax.broadcasted_iota(jnp.int32, (S, E), 1), 1.0, 0.0
    )
    spread_b = spread.astype(BF16)
    match_s = jnp.dot(spread_b, match_b, preferred_element_type=F32)
    before_s = jnp.dot(spread_b, before, preferred_element_type=F32)
    weight_s = jnp.dot(spread_b, weight.astype(BF16), preferred_element_type=F32)
    slot_of = lax.rem(lax.broadcasted_iota(jnp.int32, (S, T), 0), CAP).astype(F32)
    chosen = jnp.where((match_s > 0.5) & (before_s == slot_of), 1.0, 0.0)
    disp_t[...] = chosen.astype(BF16)
    token_copy.wait()
    for copy in weight_copies + down_copies:
        copy.start()

    def scaled(at):
        lo, w = at
        gain = gain_ref[pl.ds(lo, w)].astype(F32).reshape(1, w)
        return (tokens[:, pl.ds(lo, w)].astype(F32) * gain).astype(BF16)

    def to_all(src, dst, send, recv):
        def one(k, carry):
            et = peer_of(k)
            to_e(src.at[et], dst, send, recv, et).start()
            return carry

        lax.fori_loop(1, E, one, 0)

    def scale_b(c):
        nb[c][z] = scaled(B[c])

    def direct_b(c):
        for i, zt in ((0, zp), (1, zm)):
            to_z(nb[c].at[z], nb[c].at[z], zb_send.at[i, c], zb_recv.at[i, c], zt).start()

    def dispatch_a(c):
        rows = jnp.dot(disp_t[...], scaled(A[c]), preferred_element_type=F32).astype(BF16)
        out_a[c][...] = rows.reshape(E, CAP, A[c][1])
        to_all(out_a[c], xa[c].at[z, e], da_send.at[c], da_recv.at[c])
        xa[c][z, e] = out_a[c][e]

    def squares():
        TP = max(T, 128)
        values = tokens[...].astype(F32)
        part = jnp.sum(values * values, axis=1, keepdims=True)
        if T < 128:
            part = jnp.concatenate([part, jnp.zeros((128 - T, 1), F32)], axis=0)
        part_t = jnp.transpose(jnp.broadcast_to(part, (TP, 128)))
        sq_buf[z] = part_t[0:8, :]
        for copy in sq_copies:
            copy.start()

    sq_copies = [
        to_z(sq_buf.at[z], sq_buf.at[z], sq_send.at[dz - 1], sq_recv.at[dz - 1], lax.rem(z + dz, NZ))
        for dz in range(1, NZ)
    ]

    def prepare():
        comb[...] = jnp.transpose(chosen * weight_s).astype(BF16)
        acc_g[...] = jnp.zeros_like(acc_g)
        acc_u[...] = jnp.zeros_like(acc_u)

    def lane_of_slot():
        lane = lax.broadcasted_iota(jnp.int32, (S, 128), 1)
        return lane == lax.rem(lax.broadcasted_iota(jnp.int32, (S, 128), 0), CAP)

    def send_scales():
        for copy in sq_copies:
            copy.wait()
        total = (sq_buf[0] + sq_buf[1] + sq_buf[2] + sq_buf[3])[0:1, 0:T]
        inverse = lax.rsqrt(total / cfg["D"] + epsilon)
        per_slot = jnp.sum(disp_t[...].astype(F32) * inverse, axis=1, keepdims=True)
        laned = jnp.where(lane_of_slot(), per_slot, 0.0)
        owner = jnp.where(
            lax.broadcasted_iota(jnp.int32, (E, S), 1) // CAP == lax.broadcasted_iota(jnp.int32, (E, S), 0), 1.0, 0.0
        )
        table = jnp.dot(owner, laned, preferred_element_type=F32, precision=lax.Precision.HIGHEST)
        sc_out[...] = table.reshape(E, 1, 128)
        to_all(sc_out, sc_in.at[e], sc_send.at[0], sc_recv.at[0])
        sc_in[e] = sc_out[e]

    def take_scales():
        take(sc_in.at[pl.ds(0, E - 1)], sc_recv.at[0])
        owner = jnp.where(
            lax.broadcasted_iota(jnp.int32, (S, E), 0) // CAP == lax.broadcasted_iota(jnp.int32, (S, E), 1), 1.0, 0.0
        )
        rows = jnp.dot(
            owner, sc_in[...].reshape(E, 128), preferred_element_type=F32, precision=lax.Precision.HIGHEST
        )
        per_row = jnp.sum(jnp.where(lane_of_slot(), rows, 0.0), axis=1, keepdims=True)
        scales[...] = jnp.broadcast_to(per_row, (S, 128))

    def forward_b(c):
        lo, hi = pl.ds(0, TH), pl.ds(TH, TH)
        take(nb[c].at[zm], zb_recv.at[0, c])
        to_z(nb[c].at[zm, lo], nb[c].at[zm, lo], zb_send.at[2, c], zb_recv.at[2, c], zp).start()
        take(nb[c].at[zp], zb_recv.at[1, c])
        to_z(nb[c].at[zp, hi], nb[c].at[zp, hi], zb_send.at[3, c], zb_recv.at[3, c], zm).start()

    def dispatch_b(c):
        take(nb[c].at[zf, pl.ds(0, TH)], zb_recv.at[2, c])
        take(nb[c].at[zf, pl.ds(TH, TH)], zb_recv.at[3, c])
        for q in range(NZ):
            rows = jnp.dot(disp_t[...], nb[c][q], preferred_element_type=F32).astype(BF16)
            out_b[c][:, q] = rows.reshape(E, CAP, B[c][1])
        to_all(out_b[c], xb[c].at[e], db_send.at[c], db_recv.at[c])
        xb[c][e] = out_b[c][e]

    def direct_a(c):
        take(xa[c].at[z, pl.ds(0, E - 1)], da_recv.at[c])
        for i, zt in ((0, zp), (1, zm)):
            to_z(xa[c].at[z], xa[c].at[z], za_send.at[i, c], za_recv.at[i, c], zt).start()

    def forward_a(c):
        lo, hi = pl.ds(0, EH), pl.ds(EH, EH)
        take(xa[c].at[zm], za_recv.at[0, c])
        to_z(xa[c].at[zm, lo], xa[c].at[zm, lo], za_send.at[2, c], za_recv.at[2, c], zp).start()
        take(xa[c].at[zp], za_recv.at[1, c])
        to_z(xa[c].at[zp, hi], xa[c].at[zp, hi], za_send.at[3, c], za_recv.at[3, c], zm).start()

    def multiply(blocks, at):
        base, width = at
        x = jnp.concatenate([b.reshape(S, width) for b, _ in blocks], axis=1)
        for w_ref, acc in ((wg, acc_g), (wu, acc_u)):
            w = jnp.concatenate(
                [w_ref[pl.ds(pl.multiple_of(q * DZ + base, 128), width), :] for _, q in blocks], axis=0
            )
            acc[...] += jnp.dot(x, w, preferred_element_type=F32)

    def multiply_near(c):
        multiply([(xa[c][q], q) for q in (z, zp, zm)], A[c])

    def multiply_far(c):
        take(xa[c].at[zf, pl.ds(0, EH)], za_recv.at[2, c])
        take(xa[c].at[zf, pl.ds(EH, EH)], za_recv.at[3, c])
        multiply([(xa[c][zf], zf)], A[c])

    def multiply_b(c):
        take(xb[c].at[pl.ds(0, E - 1)], db_recv.at[c])
        multiply([(xb[c][:, q], q) for q in range(NZ)], B[c])

    def wait_weights():
        for copy in weight_copies:
            copy.wait()

    def enter():
        pl.semaphore_wait(barrier, E - 1 + NZ - 1)

    def run(plan):
        for name, *index in plan:
            with jax.named_scope(name):
                steps[name](*index)

    steps = dict(
        (fn.__name__, fn)
        for fn in (
            enter, scale_b, direct_b, dispatch_a, squares, prepare, send_scales, take_scales, forward_b,
            dispatch_b, direct_a, forward_a, multiply_near, multiply_far, multiply_b, wait_weights,
        )
    )
    run(cfg["OUT_PLAN"])

    s = scales[:, 0:1]
    g = acc_g[...] * s
    hid[...] = (g / (1.0 + jnp.exp(-g)) * (acc_u[...] * s)).astype(BF16)
    for copy in down_copies:
        copy.wait()

    def down(q, at):
        lo, w = at
        ds = pl.ds(pl.multiple_of(q * DZ + lo, 128), w)
        return jnp.dot(hid[...], wd[:, ds], preferred_element_type=F32).astype(BF16)

    lo_s, hi_s = pl.ds(0, SH), pl.ds(SH, SH)
    lo_t, hi_t = pl.ds(0, TH), pl.ds(TH, TH)

    def plus(a, b):
        return (a.astype(F32) + b.astype(F32)).astype(BF16)

    def far_part_a(c):
        far_a[c][...] = down(zf, A[c])
        to_z(far_a[c].at[lo_s], far_in_a[c].at[lo_s], ra_send.at[0, c], ra_recv.at[0, c], zp).start()
        to_z(far_a[c].at[hi_s], far_in_a[c].at[hi_s], ra_send.at[1, c], ra_recv.at[1, c], zm).start()

    def near_part_a(c):
        near_a[c][0] = down(zp, A[c])
        near_a[c][1] = down(zm, A[c])
        take(far_in_a[c].at[lo_s], ra_recv.at[0, c])
        near_a[c][0, lo_s] = plus(near_a[c][0, lo_s], far_in_a[c][lo_s])
        to_z(near_a[c].at[0], near_in_a[c].at[0], ra_send.at[2, c], ra_recv.at[2, c], zp).start()
        take(far_in_a[c].at[hi_s], ra_recv.at[1, c])
        near_a[c][1, hi_s] = plus(near_a[c][1, hi_s], far_in_a[c][hi_s])
        to_z(near_a[c].at[1], near_in_a[c].at[1], ra_send.at[3, c], ra_recv.at[3, c], zm).start()

    def own_part_a(c):
        own = down(z, A[c]).astype(F32)
        take(near_in_a[c].at[0], ra_recv.at[2, c])
        take(near_in_a[c].at[1], ra_recv.at[3, c])
        own = own + near_in_a[c][0].astype(F32) + near_in_a[c][1].astype(F32)
        out_a[c][...] = own.astype(BF16).reshape(E, CAP, A[c][1])
        to_all(out_a[c], ret_a[c].at[e], ya_send.at[c], ya_recv.at[c])
        ret_a[c][e] = out_a[c][e]

    def part_b(c):
        for q in range(NZ):
            out_b[c][:, q] = down(q, B[c]).reshape(E, CAP, B[c][1])
        to_all(out_b[c], ret_b[c].at[e], yb_send.at[c], yb_recv.at[c])
        ret_b[c][e] = out_b[c][e]

    def weigh_b(c, q):
        return jnp.dot(comb[...], ret_b[c][:, q].reshape(S, B[c][1]), preferred_element_type=F32)

    def far_part_b(c):
        take(ret_b[c].at[pl.ds(0, E - 1)], yb_recv.at[c])
        far_b[c][...] = weigh_b(c, zf).astype(BF16)
        to_z(far_b[c].at[lo_t], far_in_b[c].at[lo_t], rb_send.at[0, c], rb_recv.at[0, c], zp).start()
        to_z(far_b[c].at[hi_t], far_in_b[c].at[hi_t], rb_send.at[1, c], rb_recv.at[1, c], zm).start()

    def near_part_b(c):
        near_b[c][0] = weigh_b(c, zp).astype(BF16)
        near_b[c][1] = weigh_b(c, zm).astype(BF16)
        take(far_in_b[c].at[lo_t], rb_recv.at[0, c])
        near_b[c][0, lo_t] = plus(near_b[c][0, lo_t], far_in_b[c][lo_t])
        to_z(near_b[c].at[0], near_in_b[c].at[0], rb_send.at[2, c], rb_recv.at[2, c], zp).start()
        take(far_in_b[c].at[hi_t], rb_recv.at[1, c])
        near_b[c][1, hi_t] = plus(near_b[c][1, hi_t], far_in_b[c][hi_t])
        to_z(near_b[c].at[1], near_in_b[c].at[1], rb_send.at[3, c], rb_recv.at[3, c], zm).start()

    def own_part_b(c):
        own = weigh_b(c, z)
        take(near_in_b[c].at[0], rb_recv.at[2, c])
        take(near_in_b[c].at[1], rb_recv.at[3, c])
        own = own + near_in_b[c][0].astype(F32) + near_in_b[c][1].astype(F32)
        out_ref[:, pl.ds(*B[c])] = own.astype(BF16)

    def combine_a(c):
        take(ret_a[c].at[pl.ds(0, E - 1)], ya_recv.at[c])
        got = jnp.dot(comb[...], ret_a[c][...].reshape(S, A[c][1]), preferred_element_type=F32)
        out_ref[:, pl.ds(*A[c])] = got.astype(BF16)

    rest = pl.ds(0, E - 1)
    for c in range(NA):
        take(out_a[c].at[rest], da_send.at[c])
    for c in range(NB):
        take(out_b[c].at[rest], db_send.at[c])
    take(sc_out.at[rest], sc_send.at[0])

    steps.update(
        (fn.__name__, fn)
        for fn in (far_part_a, near_part_a, own_part_a, part_b, far_part_b, near_part_b, own_part_b, combine_a)
    )
    run(cfg["BACK_PLAN"])

    for c in range(NA):
        for i in range(2):
            take(xa[c].at[0], za_send.at[i, c])
            take(xa[c].at[0, pl.ds(0, EH)], za_send.at[2 + i, c])
            take(far_a[c].at[lo_s], ra_send.at[i, c])
            take(near_a[c].at[0], ra_send.at[2 + i, c])
        take(out_a[c].at[rest], ya_send.at[c])
    for c in range(NB):
        for i in range(2):
            take(nb[c].at[0], zb_send.at[i, c])
            take(nb[c].at[0, pl.ds(0, TH)], zb_send.at[2 + i, c])
            take(far_b[c].at[lo_t], rb_send.at[i, c])
            take(near_b[c].at[0], rb_send.at[2 + i, c])
        take(out_b[c].at[rest], yb_send.at[c])


OUT_PLAN = (
    "scale_b 0",
    "scale_b 1",
    "enter",
    "direct_b 0",
    "direct_b 1",
    "dispatch_a 0",
    "dispatch_a 1",
    "dispatch_a 2",
    "squares",
    "scale_b 2",
    "forward_b 0",
    "direct_b 2",
    "dispatch_a 3",
    "dispatch_a 4",
    "prepare",
    "forward_b 1",
    "dispatch_b 0",
    "direct_a 0",
    "forward_b 2",
    "send_scales",
    "dispatch_b 1",
    "direct_a 1",
    "dispatch_b 2",
    "wait_weights",
    "forward_a 0",
    "direct_a 2",
    "multiply_near 0",
    "forward_a 1",
    "direct_a 3",
    "multiply_near 1",
    "multiply_far 0",
    "take_scales",
    "multiply_b 0",
    "forward_a 2",
    "direct_a 4",
    "multiply_near 2",
    "multiply_far 1",
    "multiply_b 1",
    "forward_a 3",
    "multiply_near 3",
    "multiply_far 2",
    "forward_a 4",
    "multiply_near 4",
    "multiply_b 2",
    "multiply_far 3",
    "multiply_far 4",
)
BACK_PLAN = (
    "far_part_a 0",
    "part_b 0",
    "far_part_a 1",
    "part_b 1",
    "near_part_a 0",
    "far_part_a 2",
    "part_b 2",
    "near_part_a 1",
    "own_part_a 0",
    "far_part_b 0",
    "far_part_a 3",
    "near_part_a 2",
    "near_part_b 0",
    "own_part_a 1",
    "far_part_a 4",
    "near_part_a 3",
    "own_part_a 2",
    "far_part_b 1",
    "near_part_a 4",
    "near_part_b 1",
    "own_part_a 3",
    "far_part_b 2",
    "own_part_a 4",
    "near_part_b 2",
    "combine_a 0",
    "combine_a 1",
    "combine_a 2",
    "own_part_b 0",
    "own_part_b 1",
    "combine_a 3",
    "combine_a 4",
    "own_part_b 2",
)


def steps_of(text, na, nb):
    plan = []
    for step in text:
        name, *index = step.split(" ")
        index = [int(i) for i in index]
        if index and index[0] >= (nb if name.endswith("_b") else na):
            continue
        plan.append((name, *index))
    return plan


def local(cfg, tokens, norm_gain, expert_ids, gate_prob, w_gate, w_up, w_down):
    E, T, A, B = cfg["E"], cfg["T"], cfg["A"], cfg["B"]
    DZ, FFD = cfg["DZ"], cfg["FFD"]
    S = E * CAP
    vmem = pl.BlockSpec(memory_space=pltpu.VMEM)
    hbm = pl.BlockSpec(memory_space=pl.ANY)
    TP = max(T, 128)
    dma = pltpu.SemaphoreType.DMA

    def each(chunks, *shape):
        return [pltpu.VMEM((*shape, w), BF16) for _, w in chunks]

    def sems(n):
        return [dma((n,)), dma((n,)), dma((4, n)), dma((4, n)), dma((4, n)), dma((4, n)), dma((n,)), dma((n,))]

    scratch = [
        pltpu.VMEM((T, DZ), BF16),
        pltpu.VMEM((E, 1, 128), F32),
        pltpu.VMEM((E, 1, 128), F32),
        pltpu.VMEM((S, 128), F32),
        pltpu.VMEM((NZ * DZ, FFD), BF16),
        pltpu.VMEM((NZ * DZ, FFD), BF16),
        pltpu.VMEM((FFD, NZ * DZ), BF16),
        pltpu.VMEM((NZ, 8, TP), F32),
        pltpu.VMEM((S, T), BF16),
        pltpu.VMEM((T, S), BF16),
        pltpu.VMEM((S, FFD), F32),
        pltpu.VMEM((S, FFD), F32),
        pltpu.VMEM((S, FFD), BF16),
        dma,
        dma((3, WEIGHT_PIECES)),
        dma((1,)),
        dma((1,)),
        dma((NZ - 1,)),
        dma((NZ - 1,)),
        [
            each(A, NZ, E, CAP),
            each(A, E, CAP),
            each(A, S),
            each(A, S),
            each(A, 2, S),
            each(A, 2, S),
            each(A, E, CAP),
        ],
        [
            each(B, E, NZ, CAP),
            each(B, NZ, T),
            each(B, E, NZ, CAP),
            each(B, E, NZ, CAP),
            each(B, T),
            each(B, T),
            each(B, 2, T),
            each(B, 2, T),
        ],
        sems(len(A)),
        sems(len(B)),
    ]
    return pl.pallas_call(
        functools.partial(moe_kernel, cfg),
        out_shape=jax.ShapeDtypeStruct((T, DZ), BF16),
        in_specs=[hbm, vmem, vmem, vmem, hbm, hbm, hbm],
        out_specs=vmem,
        scratch_shapes=scratch,
        compiler_params=pltpu.CompilerParams(
            collective_id=0, has_side_effects=True, vmem_limit_bytes=cfg["VMEM"]
        ),
        name="moe_layer",
    )(tokens, norm_gain, expert_ids.T, gate_prob.T, w_gate[0], w_up[0], w_down[0])


def config(mesh, tokens=8192, width=D, ff=2048, a=WIDTHS_A, b=WIDTHS_B, nx=4):
    E = mesh.shape["ep"]
    DZ = width // NZ
    chunks, lo = [], 0
    for w in (*a, *b):
        chunks.append((lo, w))
        lo += w
    assert lo == DZ
    return dict(
        E=E,
        T=tokens // E,
        D=width,
        DZ=DZ,
        FFD=ff // NZ,
        A=chunks[: len(a)],
        B=chunks[len(a) :],
        NX=nx,
        STRIDE=11,
        VMEM=67_000_000,
        OUT_PLAN=steps_of(OUT_PLAN, len(a), len(b)),
        BACK_PLAN=steps_of(BACK_PLAN, len(a), len(b)),
    )


def build(mesh, cfg):
    placed = (
        P("ep", "tp"),
        P("tp"),
        P("ep", None),
        P("ep", None),
        P("ep", None, "tp"),
        P("ep", None, "tp"),
        P("ep", "tp", None),
    )
    return jax.shard_map(
        functools.partial(local, cfg), mesh=mesh, in_specs=placed, out_specs=P("ep", "tp"), check_vma=False
    )


def solution(mesh):
    return build(mesh, config(mesh))
```

```python
import functools

import jax
import jax.numpy as jnp
from jax import lax
from jax.experimental import pallas as pl
from jax.experimental.pallas import tpu as pltpu
from jax.sharding import PartitionSpec as P

MESH = pl.DeviceIdType.MESH
F32 = jnp.float32
BF16 = jnp.bfloat16

D = 7168
CAP = 16
CORES = 2
NZ = 4
WIDTHS_A = (256, 256, 256, 256)
WIDTHS_B = (256, 256, 256)
WEIGHT_PIECES = 4
epsilon = 1e-06


def moe_kernel(
    cfg,
    tokens_hbm,
    gain_hbm,
    ids_hbm,
    prob_hbm,
    wg_hbm,
    wu_hbm,
    wd_hbm,
    out_hbm,
    tokens,
    gain_ref,
    ids_ref,
    prob_ref,
    out_v,
    sc_out,
    sc_in,
    scales,
    wg,
    wu,
    wd,
    sq_buf,
    disp_t,
    comb,
    acc_g,
    acc_u,
    hid,
    t_sem,
    o_sem,
    w_sem,
    sent,
    sc_recv,
    sq_recv,
    per_a,
    per_b,
    sem_a,
    sem_b,
):
    xa, out_a, far_a, far_in_a, near_a, near_in_a, back_a, ret_a = per_a
    xb, nb, out_b, back_b, ret_b, far_b, far_in_b, near_b, near_in_b = per_b
    da_recv, za_recv, ra_recv, ya_recv = sem_a
    db_recv, zb_recv, rb_recv, yb_recv = sem_b
    da_send, db_send, za_send, zb_send, ra_send, rb_send, ya_send, yb_send, sc_send, sq_send = (
        sent.at[i] for i in range(10)
    )
    E, A, B = cfg["E"], cfg["A"], cfg["B"]
    NA, NB = len(A), len(B)
    DZ, T = cfg["DZ"], cfg["T"]
    S = E * CAP
    EH, EQ = E // 2, E // 4
    SH, SQ = S // 2, S // 4
    TH = T // 2
    e = lax.axis_index("ep")
    z = lax.axis_index("tp")
    zp = lax.rem(z + 1, NZ)
    zm = lax.rem(z + 3, NZ)
    zf = lax.rem(z + 2, NZ)

    def moved(off, sign):
        off = jnp.int32(off)
        nx, ny = cfg["NX"], E // CORES // cfg["NX"]
        mine, step = e // CORES, off // CORES
        py = lax.rem(mine // nx + sign * (step // nx) + ny, ny)
        px = lax.rem(lax.rem(mine, nx) + sign * lax.rem(step, nx) + nx, nx)
        core = lax.rem(lax.rem(e, CORES) + sign * lax.rem(off, CORES) + CORES, CORES)
        return (py * nx + px) * CORES + core

    def peer_of(k):
        return moved(lax.rem(k * cfg["STRIDE"], E), 1)

    def origin_of(k):
        return moved(lax.rem(k * cfg["STRIDE"], E), -1)

    def to_z(src, dst, send, recv, zt):
        return pltpu.make_async_remote_copy(
            src_ref=src, dst_ref=dst, send_sem=send, recv_sem=recv, device_id=(e, zt), device_id_type=MESH
        )

    def to_e(src, dst, send, recv, et):
        return pltpu.make_async_remote_copy(
            src_ref=src, dst_ref=dst, send_sem=send, recv_sem=recv, device_id=(et, z), device_id_type=MESH
        )

    def take(ref, sem):
        pltpu.make_async_copy(ref, ref, sem).wait()

    small_copies = [
        pltpu.make_async_copy(src, dst, t_sem.at[n])
        for n, (src, dst) in enumerate(
            ((ids_hbm, ids_ref), (prob_hbm, prob_ref), (gain_hbm, gain_ref), (tokens_hbm, tokens))
        )
    ]
    for copy in small_copies:
        copy.start()
    barrier = pltpu.get_barrier_semaphore()

    def hops(k):
        step, nx, ny = k // CORES, cfg["NX"], E // CORES // cfg["NX"]
        dx, dy = step % nx, step // nx
        return min(dx, nx - dx) + min(dy, ny - dy)

    for k in sorted(range(1, E), key=hops, reverse=True):
        pl.semaphore_signal(barrier, inc=1, device_id=(moved(k, 1), z), device_id_type=MESH)
    for dz in (2, 1, 3):
        pl.semaphore_signal(barrier, inc=1, device_id=(e, lax.rem(z + dz, NZ)), device_id_type=MESH)
    for copy in small_copies[:3]:
        copy.wait()

    rows_w = wg.shape[0] // WEIGHT_PIECES
    rows_d = wd.shape[0] // WEIGHT_PIECES
    weight_copies = []
    for p in range(WEIGHT_PIECES):
        rs = pl.ds(p * rows_w, rows_w)
        weight_copies.append(pltpu.make_async_copy(wg_hbm.at[rs], wg.at[rs], w_sem.at[0]))
        weight_copies.append(pltpu.make_async_copy(wu_hbm.at[rs], wu.at[rs], w_sem.at[1]))
    down_copies = []
    for p in range(WEIGHT_PIECES):
        rs = pl.ds(p * rows_d, rows_d)
        down_copies.append(pltpu.make_async_copy(wd_hbm.at[rs], wd.at[rs], w_sem.at[2]))

    ids = ids_ref[...]
    probs = prob_ref[...].astype(F32)
    expert_iota = lax.broadcasted_iota(jnp.int32, (E, T), 0)
    match = jnp.zeros((E, T), F32)
    weight = jnp.zeros((E, T), F32)
    for k in range(ids.shape[0]):
        hit = ids[k : k + 1, :] == expert_iota
        match = match + jnp.where(hit, 1.0, 0.0)
        weight = weight + jnp.where(hit, probs[k : k + 1, :], 0.0)
    earlier = jnp.where(
        lax.broadcasted_iota(jnp.int32, (T, T), 0) < lax.broadcasted_iota(jnp.int32, (T, T), 1), 1.0, 0.0
    ).astype(BF16)
    match_b = match.astype(BF16)
    before = jnp.dot(match_b, earlier, preferred_element_type=F32).astype(BF16)
    spread = jnp.where(
        lax.broadcasted_iota(jnp.int32, (S, E), 0) // CAP == lax.broadcasted_iota(jnp.int32, (S, E), 1), 1.0, 0.0
    )
    spread_b = spread.astype(BF16)
    match_s = jnp.dot(spread_b, match_b, preferred_element_type=F32)
    before_s = jnp.dot(spread_b, before, preferred_element_type=F32)
    weight_s = jnp.dot(spread_b, weight.astype(BF16), preferred_element_type=F32)
    slot_of = lax.rem(lax.broadcasted_iota(jnp.int32, (S, T), 0), CAP).astype(F32)
    chosen = jnp.where((match_s > 0.5) & (before_s == slot_of), 1.0, 0.0)
    disp_t[...] = chosen.astype(BF16)
    small_copies[3].wait()
    for copy in weight_copies + down_copies:
        copy.start()

    def scaled(at):
        lo, w = at
        gain = gain_ref[pl.ds(lo, w)].astype(F32).reshape(1, w)
        return (tokens[:, pl.ds(lo, w)].astype(F32) * gain).astype(BF16)

    def to_experts(src, dst, send, recv, h):
        def one(k, carry):
            et = peer_of(k)
            to_e(src.at[et], dst.at[k], send, recv, et).start()
            return carry

        lax.fori_loop(max(1, h * EH), (h + 1) * EH, one, 0)

    def to_origins(src, dst, send, recv, h):
        def one(k, carry):
            to_e(src.at[k], dst.at[e], send, recv, origin_of(k)).start()
            return carry

        lax.fori_loop(max(1, h * EH), (h + 1) * EH, one, 0)

    def half(h):
        return pl.ds(h * EH, EH)

    rest = pl.ds(0, E - 1)

    def others(h):
        return pl.ds(0, EH - 1 if h == 0 else EH)

    def scale_b(c):
        nb[c][z] = scaled(B[c])

    def direct_b(c):
        for i, zt in ((0, zp), (1, zm)):
            to_z(nb[c].at[z], nb[c].at[z], zb_send, zb_recv.at[0, c], zt).start()

    def dispatch_a(c, h):
        if h == 0:
            rows = jnp.dot(disp_t[...], scaled(A[c]), preferred_element_type=F32).astype(BF16)
            out_a[c][...] = rows.reshape(E, CAP, A[c][1])
        to_experts(out_a[c], xa[c].at[z], da_send, da_recv.at[c, h], h)
        if h == 0:
            xa[c][z, 0] = out_a[c][e]

    def squares():
        TP = max(T, 128)
        values = tokens[...].astype(F32)
        part = jnp.sum(values * values, axis=1, keepdims=True)
        if T < 128:
            part = jnp.concatenate([part, jnp.zeros((128 - T, 1), F32)], axis=0)
        part_t = jnp.transpose(jnp.broadcast_to(part, (TP, 128)))
        sq_buf[z] = part_t[0:8, :]
        for copy in sq_copies:
            copy.start()

    sq_copies = [
        to_z(sq_buf.at[z], sq_buf.at[z], sq_send, sq_recv.at[0], lax.rem(z + dz, NZ))
        for dz in range(1, NZ)
    ]

    def prepare():
        comb[...] = jnp.transpose(chosen * weight_s).astype(BF16)
        acc_g[...] = jnp.zeros_like(acc_g)
        acc_u[...] = jnp.zeros_like(acc_u)

    def lane_of_slot():
        lane = lax.broadcasted_iota(jnp.int32, (S, 128), 1)
        return lane == lax.rem(lax.broadcasted_iota(jnp.int32, (S, 128), 0), CAP)

    def send_scales():
        take(sq_buf.at[pl.ds(0, NZ - 1)], sq_recv.at[0])
        total = (sq_buf[0] + sq_buf[1] + sq_buf[2] + sq_buf[3])[0:1, 0:T]
        inverse = lax.rsqrt(total / cfg["D"] + epsilon)
        per_slot = jnp.sum(disp_t[...].astype(F32) * inverse, axis=1, keepdims=True)
        laned = jnp.where(lane_of_slot(), per_slot, 0.0)
        owner = jnp.where(
            lax.broadcasted_iota(jnp.int32, (E, S), 1) // CAP == lax.broadcasted_iota(jnp.int32, (E, S), 0), 1.0, 0.0
        )
        table = jnp.dot(owner, laned, preferred_element_type=F32, precision=lax.Precision.HIGHEST)
        sc_out[...] = table.reshape(E, 1, 128)
        for h in range(2):
            to_experts(sc_out, sc_in, sc_send, sc_recv.at[h], h)
        sc_in[0] = sc_out[e]

    def take_scales():
        for h in range(2):
            take(sc_in.at[others(h)], sc_recv.at[h])
        owner = jnp.where(
            lax.broadcasted_iota(jnp.int32, (S, E), 0) // CAP == lax.broadcasted_iota(jnp.int32, (S, E), 1), 1.0, 0.0
        )
        rows = jnp.dot(
            owner, sc_in[...].reshape(E, 128), preferred_element_type=F32, precision=lax.Precision.HIGHEST
        )
        per_row = jnp.sum(jnp.where(lane_of_slot(), rows, 0.0), axis=1, keepdims=True)
        scales[...] = jnp.broadcast_to(per_row, (S, 128))

    def forward_b(c):
        lo, hi = pl.ds(0, TH), pl.ds(TH, TH)
        take(nb[c].at[pl.ds(0, 2)], zb_recv.at[0, c])
        to_z(nb[c].at[zm, lo], nb[c].at[zm, lo], zb_send, zb_recv.at[1, c], zp).start()
        to_z(nb[c].at[zp, hi], nb[c].at[zp, hi], zb_send, zb_recv.at[1, c], zm).start()

    def dispatch_b(c, h):
        if h == 0:
            take(nb[c].at[zf], zb_recv.at[1, c])
            for q in range(NZ):
                rows = jnp.dot(disp_t[...], nb[c][q], preferred_element_type=F32).astype(BF16)
                out_b[c][:, q] = rows.reshape(E, CAP, B[c][1])
        to_experts(out_b[c], xb[c], db_send, db_recv.at[c, h], h)
        if h == 0:
            xb[c][0] = out_b[c][e]

    def direct_a(c, h):
        take(xa[c].at[z, others(h)], da_recv.at[c, h])
        rows = xa[c].at[z, half(h)]
        for i, zt in ((0, zp), (1, zm)):
            to_z(rows, rows, za_send, za_recv.at[0, c, h], zt).start()

    def forward_a(c, h):
        take(xa[c].at[pl.ds(0, 2), half(h)], za_recv.at[0, c, h])
        rows = xa[c].at[zm, pl.ds(h * EH, EQ)]
        to_z(rows, rows, za_send, za_recv.at[1, c, h], zp).start()
        rows = xa[c].at[zp, pl.ds(h * EH + EQ, EQ)]
        to_z(rows, rows, za_send, za_recv.at[1, c, h], zm).start()

    def multiply(blocks, at, h):
        base, width = at
        x = jnp.concatenate([b.reshape(SH, width) for b, _ in blocks], axis=1)
        for w_ref, acc in ((wg, acc_g), (wu, acc_u)):
            w = jnp.concatenate(
                [w_ref[pl.ds(pl.multiple_of(q * DZ + base, 128), width), :] for _, q in blocks], axis=0
            )
            acc[half_rows(h)] += jnp.dot(x, w, preferred_element_type=F32)

    def half_rows(h):
        return pl.ds(h * SH, SH)

    def multiply_near(c, h):
        multiply([(xa[c][q, half(h)], q) for q in (z, zp, zm)], A[c], h)

    def multiply_far(c, h):
        take(xa[c].at[zf, half(h)], za_recv.at[1, c, h])
        multiply([(xa[c][zf, half(h)], zf)], A[c], h)

    def multiply_b(c, h):
        take(xb[c].at[others(h)], db_recv.at[c, h])
        multiply([(xb[c][half(h), q], q) for q in range(NZ)], B[c], h)

    def wait_weights():
        take(wg, w_sem.at[0])
        take(wu, w_sem.at[1])

    def enter():
        pl.semaphore_wait(barrier, E - 1 + NZ - 1)

    def hidden(h):
        rows = half_rows(h)
        scale = scales[rows, 0:1]
        g = acc_g[rows] * scale
        hid[rows] = (g / (1.0 + jnp.exp(-g)) * (acc_u[rows] * scale)).astype(BF16)

    def wait_down():
        take(wd, w_sem.at[2])

    def down(q, at, h):
        lo, w = at
        ds = pl.ds(pl.multiple_of(q * DZ + lo, 128), w)
        return jnp.dot(hid[half_rows(h)], wd[:, ds], preferred_element_type=F32).astype(BF16)

    lo_t, hi_t = pl.ds(0, TH), pl.ds(TH, TH)

    def plus(a, b):
        return (a.astype(F32) + b.astype(F32)).astype(BF16)

    def quarters(h):
        return pl.ds(h * SH, SQ), pl.ds(h * SH + SQ, SQ)

    def far_part_a(c, h):
        lo, hi = quarters(h)
        far_a[c][half_rows(h)] = down(zf, A[c], h)
        to_z(far_a[c].at[lo], far_in_a[c].at[lo], ra_send, ra_recv.at[0, c, h], zp).start()
        to_z(far_a[c].at[hi], far_in_a[c].at[hi], ra_send, ra_recv.at[0, c, h], zm).start()

    def near_part_a(c, h):
        lo, hi = quarters(h)
        rows = half_rows(h)
        near_a[c][0, rows] = down(zp, A[c], h)
        near_a[c][1, rows] = down(zm, A[c], h)
        take(far_in_a[c].at[rows], ra_recv.at[0, c, h])
        near_a[c][0, lo] = plus(near_a[c][0, lo], far_in_a[c][lo])
        to_z(near_a[c].at[0, rows], near_in_a[c].at[0, rows], ra_send, ra_recv.at[1, c, h], zp).start()
        near_a[c][1, hi] = plus(near_a[c][1, hi], far_in_a[c][hi])
        to_z(near_a[c].at[1, rows], near_in_a[c].at[1, rows], ra_send, ra_recv.at[1, c, h], zm).start()

    def own_part_a(c, h):
        rows = half_rows(h)
        own = down(z, A[c], h).astype(F32)
        take(near_in_a[c].at[:, rows], ra_recv.at[1, c, h])
        own = own + near_in_a[c][0, rows].astype(F32) + near_in_a[c][1, rows].astype(F32)
        back_a[c][half(h)] = own.astype(BF16).reshape(EH, CAP, A[c][1])
        to_origins(back_a[c], ret_a[c], ya_send, ya_recv.at[c], h)
        if h == 0:
            ret_a[c][e] = back_a[c][0]

    def part_b(c, h):
        for q in range(NZ):
            back_b[c][half(h), q] = down(q, B[c], h).reshape(EH, CAP, B[c][1])
        to_origins(back_b[c], ret_b[c], yb_send, yb_recv.at[c], h)
        if h == 0:
            ret_b[c][e] = back_b[c][0]

    def weigh_b(c, q):
        return jnp.dot(comb[...], ret_b[c][:, q].reshape(S, B[c][1]), preferred_element_type=F32)

    def far_part_b(c):
        take(ret_b[c].at[rest], yb_recv.at[c])
        far_b[c][...] = weigh_b(c, zf).astype(BF16)
        to_z(far_b[c].at[lo_t], far_in_b[c].at[lo_t], rb_send, rb_recv.at[0, c], zp).start()
        to_z(far_b[c].at[hi_t], far_in_b[c].at[hi_t], rb_send, rb_recv.at[0, c], zm).start()

    def near_part_b(c):
        near_b[c][0] = weigh_b(c, zp).astype(BF16)
        near_b[c][1] = weigh_b(c, zm).astype(BF16)
        take(far_in_b[c], rb_recv.at[0, c])
        near_b[c][0, lo_t] = plus(near_b[c][0, lo_t], far_in_b[c][lo_t])
        to_z(near_b[c].at[0], near_in_b[c].at[0], rb_send, rb_recv.at[1, c], zp).start()
        near_b[c][1, hi_t] = plus(near_b[c][1, hi_t], far_in_b[c][hi_t])
        to_z(near_b[c].at[1], near_in_b[c].at[1], rb_send, rb_recv.at[1, c], zm).start()

    def own_part_b(c):
        own = weigh_b(c, z)
        take(near_in_b[c], rb_recv.at[1, c])
        own = own + near_in_b[c][0].astype(F32) + near_in_b[c][1].astype(F32)
        out_v[:, pl.ds(*B[c])] = own.astype(BF16)
        write_out(NA + c).start()

    def write_out(n):
        at = pl.ds(*(A + B)[n])
        return pltpu.make_async_copy(out_v.at[:, at], out_hbm.at[:, at], o_sem)

    def combine_a(c):
        take(ret_a[c].at[rest], ya_recv.at[c])
        got = jnp.dot(comb[...], ret_a[c][...].reshape(S, A[c][1]), preferred_element_type=F32)
        out_v[:, pl.ds(*A[c])] = got.astype(BF16)
        write_out(c).start()

    order = (
        (scale_b, 0), (scale_b, 1), (scale_b, 2), (enter,), (direct_b, 0), (dispatch_a, 0, 0), (direct_b, 1),
        (dispatch_a, 0, 1), (direct_b, 2), (dispatch_a, 1, 0), (dispatch_a, 1, 1), (squares,), (dispatch_a, 2, 0),
        (dispatch_a, 2, 1), (forward_b, 0), (dispatch_a, 3, 0), (dispatch_a, 3, 1), (prepare,), (forward_b, 1),
        (direct_a, 0, 0), (direct_a, 0, 1), (forward_b, 2), (send_scales,), (dispatch_b, 0, 0), (dispatch_b, 0, 1),
        (direct_a, 1, 0), (direct_a, 1, 1), (dispatch_b, 1, 0), (dispatch_b, 1, 1), (wait_weights,),
        (forward_a, 0, 0), (direct_a, 2, 0), (forward_a, 0, 1), (direct_a, 2, 1), (dispatch_b, 2, 0),
        (dispatch_b, 2, 1), (multiply_near, 0, 0), (multiply_near, 0, 1), (forward_a, 1, 0), (direct_a, 3, 0),
        (forward_a, 1, 1), (direct_a, 3, 1), (multiply_far, 0, 0), (multiply_far, 0, 1), (multiply_near, 1, 0),
        (multiply_near, 1, 1), (take_scales,), (multiply_b, 0, 0), (multiply_far, 1, 0), (multiply_b, 0, 1),
        (forward_a, 2, 0), (multiply_near, 2, 0), (forward_a, 2, 1), (multiply_far, 1, 1), (multiply_near, 2, 1),
        (multiply_b, 1, 0), (multiply_b, 1, 1), (forward_a, 3, 0), (multiply_near, 3, 0), (multiply_far, 2, 0),
        (multiply_far, 2, 1), (wait_down,), (forward_a, 3, 1), (multiply_b, 2, 0), (multiply_near, 3, 1),
        (multiply_far, 3, 0), (hidden, 0), (part_b, 1, 0), (far_part_a, 0, 0), (part_b, 0, 0), (far_part_a, 1, 0),
        (multiply_far, 3, 1), (multiply_b, 2, 1), (hidden, 1), (far_part_a, 0, 1), (part_b, 0, 1),
        (near_part_a, 0, 0), (far_part_a, 1, 1), (part_b, 1, 1), (near_part_a, 0, 1), (far_part_a, 2, 0),
        (near_part_a, 1, 0), (part_b, 2, 0), (far_part_a, 2, 1), (part_b, 2, 1), (near_part_a, 1, 1),
        (own_part_a, 0, 0), (far_part_a, 3, 0), (near_part_a, 2, 0), (own_part_a, 0, 1), (far_part_b, 0),
        (far_part_a, 3, 1), (near_part_a, 2, 1), (own_part_a, 1, 0), (own_part_a, 1, 1), (near_part_b, 0),
        (near_part_a, 3, 1), (own_part_a, 2, 0), (far_part_b, 1), (near_part_a, 3, 0), (far_part_b, 2),
        (own_part_a, 2, 1), (near_part_b, 1), (own_part_a, 3, 0), (near_part_b, 2), (combine_a, 0),
        (own_part_a, 3, 1), (own_part_b, 0), (combine_a, 1), (own_part_b, 1), (combine_a, 2), (own_part_b, 2),
        (combine_a, 3),
    )
    for step, *at in order:
        step(*at)

    take(out_v, o_sem)
    wa, wb = (sum(w for _, w in chunks) for chunks in (A, B))
    for sem, count in (
        (da_send, (S - CAP) * wa),
        (db_send, (S - CAP) * NZ * wb),
        (za_send, 3 * S * wa),
        (zb_send, 3 * T * wb),
        (ra_send, 3 * S * wa),
        (rb_send, 3 * T * wb),
        (ya_send, (S - CAP) * wa),
        (yb_send, (S - CAP) * NZ * wb),
    ):
        take(wg.at[pl.ds(0, count // wg.shape[1])], sem)
    take(sc_out.at[rest], sc_send)
    take(sq_buf.at[pl.ds(0, NZ - 1)], sq_send)


def local(cfg, tokens, norm_gain, expert_ids, gate_prob, w_gate, w_up, w_down):
    E, T, A, B = cfg["E"], cfg["T"], cfg["A"], cfg["B"]
    DZ, FFD = cfg["DZ"], cfg["FFD"]
    S = E * CAP
    hbm = pl.BlockSpec(memory_space=pl.ANY)
    TP = max(T, 128)
    dma = pltpu.SemaphoreType.DMA

    def each(chunks, *shape):
        return [pltpu.VMEM((*shape, w), BF16) for _, w in chunks]

    na, nb = len(A), len(B)
    scratch = [
        pltpu.VMEM((T, DZ), BF16),
        pltpu.VMEM((DZ,), BF16),
        pltpu.VMEM(expert_ids.shape[::-1], jnp.int32),
        pltpu.VMEM(expert_ids.shape[::-1], BF16),
        pltpu.VMEM((T, DZ), BF16),
        pltpu.VMEM((E, 1, 128), F32),
        pltpu.VMEM((E, 1, 128), F32),
        pltpu.VMEM((S, 128), F32),
        pltpu.VMEM((NZ * DZ, FFD), BF16),
        pltpu.VMEM((NZ * DZ, FFD), BF16),
        pltpu.VMEM((FFD, NZ * DZ), BF16),
        pltpu.VMEM((NZ, 8, TP), F32),
        pltpu.VMEM((S, T), BF16),
        pltpu.VMEM((T, S), BF16),
        pltpu.VMEM((S, FFD), F32),
        pltpu.VMEM((S, FFD), F32),
        pltpu.VMEM((S, FFD), BF16),
        dma((4,)),
        dma,
        dma((3,)),
        dma((10,)),
        dma((2,)),
        dma((1,)),
        [
            each(A, NZ, E, CAP),
            each(A, E, CAP),
            each(A, S),
            each(A, S),
            each(A, 2, S),
            each(A, 2, S),
            each(A, E, CAP),
            each(A, E, CAP),
        ],
        [
            each(B, E, NZ, CAP),
            each(B, NZ, T),
            each(B, E, NZ, CAP),
            each(B, E, NZ, CAP),
            each(B, E, NZ, CAP),
            each(B, T),
            each(B, T),
            each(B, 2, T),
            each(B, 2, T),
        ],
        [dma((na, 2)), dma((2, na, 2)), dma((2, na, 2)), dma((na,))],
        [dma((nb, 2)), dma((2, nb)), dma((2, nb)), dma((nb,))],
    ]
    return pl.pallas_call(
        functools.partial(moe_kernel, cfg),
        out_shape=jax.ShapeDtypeStruct((T, DZ), BF16),
        in_specs=[hbm] * 7,
        out_specs=hbm,
        scratch_shapes=scratch,
        compiler_params=pltpu.CompilerParams(
            collective_id=0, has_side_effects=True, vmem_limit_bytes=cfg["VMEM"]
        ),
        name="moe_layer",
    )(tokens, norm_gain, expert_ids.T, gate_prob.T, w_gate[0], w_up[0], w_down[0])


def config(mesh, tokens=8192, width=D, ff=2048, a=WIDTHS_A, b=WIDTHS_B, nx=4):
    E = mesh.shape["ep"]
    DZ = width // NZ
    chunks, lo = [], 0
    for w in (*a, *b):
        chunks.append((lo, w))
        lo += w
    assert lo == DZ
    return dict(
        E=E,
        T=tokens // E,
        D=width,
        DZ=DZ,
        FFD=ff // NZ,
        A=chunks[: len(a)],
        B=chunks[len(a) :],
        NX=nx,
        STRIDE=11,
        VMEM=67_000_000,
    )


def build(mesh, cfg):
    placed = (
        P("ep", "tp"),
        P("tp"),
        P("ep", None),
        P("ep", None),
        P("ep", None, "tp"),
        P("ep", None, "tp"),
        P("ep", "tp", None),
    )
    return jax.shard_map(
        functools.partial(local, cfg), mesh=mesh, in_specs=placed, out_specs=P("ep", "tp"), check_vma=False
    )


def solution(mesh):
    return build(mesh, config(mesh))
```

```python
import functools

import jax
import jax.numpy as jnp
from jax import lax
from jax.experimental import pallas as pl
from jax.experimental.pallas import tpu as pltpu
from jax.sharding import PartitionSpec as P

MESH = pl.DeviceIdType.MESH
F32 = jnp.float32
BF16 = jnp.bfloat16

D = 7168
CAP = 16
CORES = 2
NZ = 4
WIDTHS_A = (256, 256, 256, 256)
WIDTHS_B = (256, 256, 256)
WEIGHT_PIECES = 4
epsilon = 1e-06


def moe_kernel(
    cfg,
    tokens_hbm,
    gain_hbm,
    ids_hbm,
    prob_hbm,
    wg_hbm,
    wu_hbm,
    wd_hbm,
    out_hbm,
    tokens,
    gain_ref,
    ids_ref,
    prob_ref,
    out_v,
    sc_out,
    sc_in,
    scales,
    wg,
    wu,
    wd,
    sq_buf,
    disp_t,
    comb,
    acc_g,
    acc_u,
    hid,
    t_sem,
    o_sem,
    w_sem,
    sent,
    sc_recv,
    sq_recv,
    per_a,
    per_b,
    sem_a,
    sem_b,
):
    xa, out_a, far_a, far_in_a, near_a, near_in_a, back_a, ret_a = per_a
    xb, nb, out_b, back_b, ret_b, far_b, far_in_b, near_b, near_in_b = per_b
    da_recv, za_recv, ra_recv, ya_recv = sem_a
    db_recv, zb_recv, rb_recv, yb_recv = sem_b
    da_send, db_send, za_send, zb_send, ra_send, rb_send, ya_send, yb_send, sc_send, sq_send = (
        sent.at[i] for i in range(10)
    )
    E, A, B = cfg["E"], cfg["A"], cfg["B"]
    NA, NB = len(A), len(B)
    DZ, T = cfg["DZ"], cfg["T"]
    S = E * CAP
    EH, EQ = E // 2, E // 4
    SH, SQ = S // 2, S // 4
    TH = T // 2
    e = lax.axis_index("ep")
    z = lax.axis_index("tp")
    zp = lax.rem(z + 1, NZ)
    zm = lax.rem(z + 3, NZ)
    zf = lax.rem(z + 2, NZ)

    def moved(off, sign):
        off = jnp.int32(off)
        nx, ny = cfg["NX"], E // CORES // cfg["NX"]
        mine, step = e // CORES, off // CORES
        py = lax.rem(mine // nx + sign * (step // nx) + ny, ny)
        px = lax.rem(lax.rem(mine, nx) + sign * lax.rem(step, nx) + nx, nx)
        core = lax.rem(lax.rem(e, CORES) + sign * lax.rem(off, CORES) + CORES, CORES)
        return (py * nx + px) * CORES + core

    def peer_of(k):
        return moved(lax.rem(k * cfg["STRIDE"], E), 1)

    def origin_of(k):
        return moved(lax.rem(k * cfg["STRIDE"], E), -1)

    def to_z(src, dst, send, recv, zt):
        return pltpu.make_async_remote_copy(
            src_ref=src, dst_ref=dst, send_sem=send, recv_sem=recv, device_id=(e, zt), device_id_type=MESH
        )

    def to_e(src, dst, send, recv, et):
        return pltpu.make_async_remote_copy(
            src_ref=src, dst_ref=dst, send_sem=send, recv_sem=recv, device_id=(et, z), device_id_type=MESH
        )

    def take(ref, sem):
        pltpu.make_async_copy(ref, ref, sem).wait()

    small_copies = [
        pltpu.make_async_copy(src, dst, t_sem.at[n])
        for n, (src, dst) in enumerate(
            ((ids_hbm, ids_ref), (prob_hbm, prob_ref), (gain_hbm, gain_ref), (tokens_hbm, tokens))
        )
    ]
    for copy in small_copies:
        copy.start()
    barrier = pltpu.get_barrier_semaphore()

    def hops(k):
        step, nx, ny = k // CORES, cfg["NX"], E // CORES // cfg["NX"]
        dx, dy = step % nx, step // nx
        return min(dx, nx - dx) + min(dy, ny - dy)

    for k in sorted(range(1, E), key=hops, reverse=True):
        pl.semaphore_signal(barrier, inc=1, device_id=(moved(k, 1), z), device_id_type=MESH)
    for dz in (2, 1, 3):
        pl.semaphore_signal(barrier, inc=1, device_id=(e, lax.rem(z + dz, NZ)), device_id_type=MESH)
    for copy in small_copies[:3]:
        copy.wait()

    rows_w = wg.shape[0] // WEIGHT_PIECES
    rows_d = wd.shape[0] // WEIGHT_PIECES
    weight_copies = []
    for p in range(WEIGHT_PIECES):
        rs = pl.ds(p * rows_w, rows_w)
        weight_copies.append(pltpu.make_async_copy(wg_hbm.at[rs], wg.at[rs], w_sem.at[0]))
        weight_copies.append(pltpu.make_async_copy(wu_hbm.at[rs], wu.at[rs], w_sem.at[1]))
    down_copies = []
    for p in range(WEIGHT_PIECES):
        rs = pl.ds(p * rows_d, rows_d)
        down_copies.append(pltpu.make_async_copy(wd_hbm.at[rs], wd.at[rs], w_sem.at[2]))

    ids = ids_ref[...]
    probs = prob_ref[...].astype(F32)
    expert_iota = lax.broadcasted_iota(jnp.int32, (E, T), 0)
    match = jnp.zeros((E, T), F32)
    weight = jnp.zeros((E, T), F32)
    for k in range(ids.shape[0]):
        hit = ids[k : k + 1, :] == expert_iota
        match = match + jnp.where(hit, 1.0, 0.0)
        weight = weight + jnp.where(hit, probs[k : k + 1, :], 0.0)
    earlier = jnp.where(
        lax.broadcasted_iota(jnp.int32, (T, T), 0) < lax.broadcasted_iota(jnp.int32, (T, T), 1), 1.0, 0.0
    ).astype(BF16)
    match_b = match.astype(BF16)
    before = jnp.dot(match_b, earlier, preferred_element_type=F32).astype(BF16)
    spread = jnp.where(
        lax.broadcasted_iota(jnp.int32, (S, E), 0) // CAP == lax.broadcasted_iota(jnp.int32, (S, E), 1), 1.0, 0.0
    )
    spread_b = spread.astype(BF16)
    match_s = jnp.dot(spread_b, match_b, preferred_element_type=F32)
    before_s = jnp.dot(spread_b, before, preferred_element_type=F32)
    weight_s = jnp.dot(spread_b, weight.astype(BF16), preferred_element_type=F32)
    slot_of = lax.rem(lax.broadcasted_iota(jnp.int32, (S, T), 0), CAP).astype(F32)
    chosen = jnp.where((match_s > 0.5) & (before_s == slot_of), 1.0, 0.0)
    disp_t[...] = chosen.astype(BF16)
    small_copies[3].wait()
    for copy in weight_copies + down_copies:
        copy.start()

    def scaled(at):
        lo, w = at
        gain = gain_ref[pl.ds(lo, w)].astype(F32).reshape(1, w)
        return (tokens[:, pl.ds(lo, w)].astype(F32) * gain).astype(BF16)

    def to_experts(src, dst, send, recv, h):
        def one(k, carry):
            et = peer_of(k)
            to_e(src.at[et], dst.at[k], send, recv, et).start()
            return carry

        lax.fori_loop(max(1, h * EH), (h + 1) * EH, one, 0)

    def to_origins(src, dst, send, recv, h):
        def one(k, carry):
            to_e(src.at[k], dst.at[e], send, recv, origin_of(k)).start()
            return carry

        lax.fori_loop(max(1, h * EH), (h + 1) * EH, one, 0)

    def half(h):
        return pl.ds(h * EH, EH)

    rest = pl.ds(0, E - 1)

    def others(h):
        return pl.ds(0, EH - 1 if h == 0 else EH)

    def scale_b(c):
        nb[c][z] = scaled(B[c])

    def direct_b(c):
        for i, zt in ((0, zp), (1, zm)):
            to_z(nb[c].at[z], nb[c].at[z], zb_send, zb_recv.at[0, c], zt).start()

    def dispatch_a(c, h):
        if h == 0:
            rows = jnp.dot(disp_t[...], scaled(A[c]), preferred_element_type=F32).astype(BF16)
            out_a[c][...] = rows.reshape(E, CAP, A[c][1])
        to_experts(out_a[c], xa[c].at[z], da_send, da_recv.at[c, h], h)
        if h == 0:
            xa[c][z, 0] = out_a[c][e]

    def squares():
        TP = max(T, 128)
        values = tokens[...].astype(F32)
        part = jnp.sum(values * values, axis=1, keepdims=True)
        if T < 128:
            part = jnp.concatenate([part, jnp.zeros((128 - T, 1), F32)], axis=0)
        part_t = jnp.transpose(jnp.broadcast_to(part, (TP, 128)))
        sq_buf[z] = part_t[0:8, :]
        for copy in sq_copies:
            copy.start()

    sq_copies = [
        to_z(sq_buf.at[z], sq_buf.at[z], sq_send, sq_recv.at[0], lax.rem(z + dz, NZ))
        for dz in range(1, NZ)
    ]

    def prepare():
        comb[...] = jnp.transpose(chosen * weight_s).astype(BF16)
        acc_g[...] = jnp.zeros_like(acc_g)
        acc_u[...] = jnp.zeros_like(acc_u)

    def lane_of_slot():
        lane = lax.broadcasted_iota(jnp.int32, (S, 128), 1)
        return lane == lax.rem(lax.broadcasted_iota(jnp.int32, (S, 128), 0), CAP)

    def send_scales():
        take(sq_buf.at[pl.ds(0, NZ - 1)], sq_recv.at[0])
        total = (sq_buf[0] + sq_buf[1] + sq_buf[2] + sq_buf[3])[0:1, 0:T]
        inverse = lax.rsqrt(total / cfg["D"] + epsilon)
        per_slot = jnp.sum(disp_t[...].astype(F32) * inverse, axis=1, keepdims=True)
        laned = jnp.where(lane_of_slot(), per_slot, 0.0)
        owner = jnp.where(
            lax.broadcasted_iota(jnp.int32, (E, S), 1) // CAP == lax.broadcasted_iota(jnp.int32, (E, S), 0), 1.0, 0.0
        )
        table = jnp.dot(owner, laned, preferred_element_type=F32, precision=lax.Precision.HIGHEST)
        sc_out[...] = table.reshape(E, 1, 128)
        for h in range(2):
            to_experts(sc_out, sc_in, sc_send, sc_recv.at[h], h)
        sc_in[0] = sc_out[e]

    def take_scales():
        for h in range(2):
            take(sc_in.at[others(h)], sc_recv.at[h])
        owner = jnp.where(
            lax.broadcasted_iota(jnp.int32, (S, E), 0) // CAP == lax.broadcasted_iota(jnp.int32, (S, E), 1), 1.0, 0.0
        )
        rows = jnp.dot(
            owner, sc_in[...].reshape(E, 128), preferred_element_type=F32, precision=lax.Precision.HIGHEST
        )
        per_row = jnp.sum(jnp.where(lane_of_slot(), rows, 0.0), axis=1, keepdims=True)
        scales[...] = jnp.broadcast_to(per_row, (S, 128))

    def forward_b(c):
        lo, hi = pl.ds(0, TH), pl.ds(TH, TH)
        take(nb[c].at[pl.ds(0, 2)], zb_recv.at[0, c])
        to_z(nb[c].at[zm, lo], nb[c].at[zm, lo], zb_send, zb_recv.at[1, c], zp).start()
        to_z(nb[c].at[zp, hi], nb[c].at[zp, hi], zb_send, zb_recv.at[1, c], zm).start()

    def dispatch_b(c, h):
        if h == 0:
            take(nb[c].at[zf], zb_recv.at[1, c])
            for q in range(NZ):
                rows = jnp.dot(disp_t[...], nb[c][q], preferred_element_type=F32).astype(BF16)
                out_b[c][:, q] = rows.reshape(E, CAP, B[c][1])
        to_experts(out_b[c], xb[c], db_send, db_recv.at[c, h], h)
        if h == 0:
            xb[c][0] = out_b[c][e]

    def direct_a(c, h):
        take(xa[c].at[z, others(h)], da_recv.at[c, h])
        rows = xa[c].at[z, half(h)]
        for i, zt in ((0, zp), (1, zm)):
            to_z(rows, rows, za_send, za_recv.at[0, c, h], zt).start()

    def forward_a(c, h):
        take(xa[c].at[pl.ds(0, 2), half(h)], za_recv.at[0, c, h])
        rows = xa[c].at[zm, pl.ds(h * EH, EQ)]
        to_z(rows, rows, za_send, za_recv.at[1, c, h], zp).start()
        rows = xa[c].at[zp, pl.ds(h * EH + EQ, EQ)]
        to_z(rows, rows, za_send, za_recv.at[1, c, h], zm).start()

    def multiply(blocks, at, h):
        base, width = at
        x = jnp.concatenate([b.reshape(SH, width) for b, _ in blocks], axis=1)
        for w_ref, acc in ((wg, acc_g), (wu, acc_u)):
            w = jnp.concatenate(
                [w_ref[pl.ds(pl.multiple_of(q * DZ + base, 128), width), :] for _, q in blocks], axis=0
            )
            acc[half_rows(h)] += jnp.dot(x, w, preferred_element_type=F32)

    def half_rows(h):
        return pl.ds(h * SH, SH)

    def multiply_near(c, h):
        multiply([(xa[c][q, half(h)], q) for q in (z, zp, zm)], A[c], h)

    def multiply_far(c, h):
        take(xa[c].at[zf, half(h)], za_recv.at[1, c, h])
        multiply([(xa[c][zf, half(h)], zf)], A[c], h)

    def multiply_b(c, h):
        take(xb[c].at[others(h)], db_recv.at[c, h])
        multiply([(xb[c][half(h), q], q) for q in range(NZ)], B[c], h)

    def wait_weights():
        take(wg, w_sem.at[0])
        take(wu, w_sem.at[1])

    def enter():
        pl.semaphore_wait(barrier, E - 1 + NZ - 1)

    def hidden(h):
        rows = half_rows(h)
        scale = scales[rows, 0:1]
        g = acc_g[rows] * scale
        hid[rows] = (g / (1.0 + jnp.exp(-g)) * (acc_u[rows] * scale)).astype(BF16)

    def wait_down():
        take(wd, w_sem.at[2])

    def down(q, at, h):
        lo, w = at
        ds = pl.ds(pl.multiple_of(q * DZ + lo, 128), w)
        return jnp.dot(hid[half_rows(h)], wd[:, ds], preferred_element_type=F32).astype(BF16)

    lo_t, hi_t = pl.ds(0, TH), pl.ds(TH, TH)

    def plus(a, b):
        return (a.astype(F32) + b.astype(F32)).astype(BF16)

    def quarters(h):
        return pl.ds(h * SH, SQ), pl.ds(h * SH + SQ, SQ)

    def far_part_a(c, h):
        lo, hi = quarters(h)
        far_a[c][half_rows(h)] = down(zf, A[c], h)
        to_z(far_a[c].at[lo], far_in_a[c].at[lo], ra_send, ra_recv.at[0, c, h], zp).start()
        to_z(far_a[c].at[hi], far_in_a[c].at[hi], ra_send, ra_recv.at[0, c, h], zm).start()

    def near_part_a(c, h):
        lo, hi = quarters(h)
        rows = half_rows(h)
        near_a[c][0, rows] = down(zp, A[c], h)
        near_a[c][1, rows] = down(zm, A[c], h)
        take(far_in_a[c].at[rows], ra_recv.at[0, c, h])
        near_a[c][0, lo] = plus(near_a[c][0, lo], far_in_a[c][lo])
        to_z(near_a[c].at[0, rows], near_in_a[c].at[0, rows], ra_send, ra_recv.at[1, c, h], zp).start()
        near_a[c][1, hi] = plus(near_a[c][1, hi], far_in_a[c][hi])
        to_z(near_a[c].at[1, rows], near_in_a[c].at[1, rows], ra_send, ra_recv.at[1, c, h], zm).start()

    def own_part_a(c, h):
        rows = half_rows(h)
        own = down(z, A[c], h).astype(F32)
        take(near_in_a[c].at[:, rows], ra_recv.at[1, c, h])
        own = own + near_in_a[c][0, rows].astype(F32) + near_in_a[c][1, rows].astype(F32)
        back_a[c][half(h)] = own.astype(BF16).reshape(EH, CAP, A[c][1])
        to_origins(back_a[c], ret_a[c], ya_send, ya_recv.at[c], h)
        if h == 0:
            ret_a[c][e] = back_a[c][0]

    def part_b(c, h):
        for q in range(NZ):
            back_b[c][half(h), q] = down(q, B[c], h).reshape(EH, CAP, B[c][1])
        to_origins(back_b[c], ret_b[c], yb_send, yb_recv.at[c], h)
        if h == 0:
            ret_b[c][e] = back_b[c][0]

    def weigh_b(c, q):
        return jnp.dot(comb[...], ret_b[c][:, q].reshape(S, B[c][1]), preferred_element_type=F32)

    def far_part_b(c):
        take(ret_b[c].at[rest], yb_recv.at[c])
        far_b[c][...] = weigh_b(c, zf).astype(BF16)
        to_z(far_b[c].at[lo_t], far_in_b[c].at[lo_t], rb_send, rb_recv.at[0, c], zp).start()
        to_z(far_b[c].at[hi_t], far_in_b[c].at[hi_t], rb_send, rb_recv.at[0, c], zm).start()

    def near_part_b(c):
        near_b[c][0] = weigh_b(c, zp).astype(BF16)
        near_b[c][1] = weigh_b(c, zm).astype(BF16)
        take(far_in_b[c], rb_recv.at[0, c])
        near_b[c][0, lo_t] = plus(near_b[c][0, lo_t], far_in_b[c][lo_t])
        to_z(near_b[c].at[0], near_in_b[c].at[0], rb_send, rb_recv.at[1, c], zp).start()
        near_b[c][1, hi_t] = plus(near_b[c][1, hi_t], far_in_b[c][hi_t])
        to_z(near_b[c].at[1], near_in_b[c].at[1], rb_send, rb_recv.at[1, c], zm).start()

    def own_part_b(c):
        own = weigh_b(c, z)
        take(near_in_b[c], rb_recv.at[1, c])
        own = own + near_in_b[c][0].astype(F32) + near_in_b[c][1].astype(F32)
        out_v[:, pl.ds(*B[c])] = own.astype(BF16)
        write_out(NA + c).start()

    def write_out(n):
        at = pl.ds(*(A + B)[n])
        return pltpu.make_async_copy(out_v.at[:, at], out_hbm.at[:, at], o_sem)

    def combine_a(c):
        take(ret_a[c].at[rest], ya_recv.at[c])
        got = jnp.dot(comb[...], ret_a[c][...].reshape(S, A[c][1]), preferred_element_type=F32)
        out_v[:, pl.ds(*A[c])] = got.astype(BF16)
        write_out(c).start()

    order = (
        (scale_b, 0), (scale_b, 1), (scale_b, 2), (enter,), (direct_b, 0), (dispatch_a, 0, 0), (direct_b, 1),
        (dispatch_a, 0, 1), (direct_b, 2), (dispatch_a, 1, 0), (dispatch_a, 1, 1), (squares,), (dispatch_a, 2, 0),
        (dispatch_a, 2, 1), (forward_b, 0), (dispatch_a, 3, 0), (dispatch_a, 3, 1), (prepare,), (forward_b, 1),
        (direct_a, 0, 0), (direct_a, 0, 1), (forward_b, 2), (send_scales,), (dispatch_b, 0, 0), (dispatch_b, 0, 1),
        (direct_a, 1, 0), (direct_a, 1, 1), (dispatch_b, 1, 0), (dispatch_b, 1, 1), (wait_weights,),
        (forward_a, 0, 0), (direct_a, 2, 0), (forward_a, 0, 1), (direct_a, 2, 1), (dispatch_b, 2, 0),
        (dispatch_b, 2, 1), (multiply_near, 0, 0), (multiply_near, 0, 1), (forward_a, 1, 0), (direct_a, 3, 0),
        (forward_a, 1, 1), (direct_a, 3, 1), (multiply_far, 0, 0), (multiply_far, 0, 1), (multiply_near, 1, 0),
        (multiply_near, 1, 1), (take_scales,), (multiply_b, 0, 0), (multiply_far, 1, 0), (multiply_b, 0, 1),
        (forward_a, 2, 0), (multiply_far, 1, 1), (multiply_near, 2, 0), (forward_a, 2, 1), (multiply_near, 2, 1),
        (forward_a, 3, 0), (multiply_b, 1, 0), (multiply_far, 2, 0), (multiply_b, 1, 1), (multiply_near, 3, 0),
        (multiply_far, 2, 1), (wait_down,), (forward_a, 3, 1), (multiply_b, 2, 0), (multiply_near, 3, 1),
        (multiply_far, 3, 0), (hidden, 0), (part_b, 1, 0), (far_part_a, 0, 0), (part_b, 0, 0), (far_part_a, 1, 0),
        (multiply_far, 3, 1), (multiply_b, 2, 1), (hidden, 1), (far_part_a, 0, 1), (part_b, 0, 1),
        (near_part_a, 0, 0), (far_part_a, 1, 1), (part_b, 1, 1), (near_part_a, 0, 1), (far_part_a, 2, 0),
        (near_part_a, 1, 0), (part_b, 2, 0), (far_part_a, 2, 1), (part_b, 2, 1), (near_part_a, 1, 1),
        (own_part_a, 0, 0), (far_part_a, 3, 0), (near_part_a, 2, 0), (own_part_a, 0, 1), (far_part_b, 0),
        (far_part_a, 3, 1), (near_part_a, 2, 1), (own_part_a, 1, 0), (own_part_a, 1, 1), (near_part_b, 0),
        (near_part_a, 3, 0), (own_part_a, 2, 0), (far_part_b, 1), (near_part_a, 3, 1), (own_part_a, 2, 1),
        (own_part_a, 3, 0), (far_part_b, 2), (near_part_b, 1), (own_part_a, 3, 1), (near_part_b, 2), (combine_a, 0),
        (own_part_b, 0), (combine_a, 1), (own_part_b, 1), (combine_a, 2), (own_part_b, 2), (combine_a, 3),
    )
    for step, *at in order:
        step(*at)

    take(out_v, o_sem)
    wa, wb = (sum(w for _, w in chunks) for chunks in (A, B))
    for sem, count in (
        (da_send, (S - CAP) * wa),
        (db_send, (S - CAP) * NZ * wb),
        (za_send, 3 * S * wa),
        (zb_send, 3 * T * wb),
        (ra_send, 3 * S * wa),
        (rb_send, 3 * T * wb),
        (ya_send, (S - CAP) * wa),
        (yb_send, (S - CAP) * NZ * wb),
    ):
        take(wg.at[pl.ds(0, count // wg.shape[1])], sem)
    take(sc_out.at[rest], sc_send)
    take(sq_buf.at[pl.ds(0, NZ - 1)], sq_send)


def local(cfg, tokens, norm_gain, expert_ids, gate_prob, w_gate, w_up, w_down):
    E, T, A, B = cfg["E"], cfg["T"], cfg["A"], cfg["B"]
    DZ, FFD = cfg["DZ"], cfg["FFD"]
    S = E * CAP
    hbm = pl.BlockSpec(memory_space=pl.ANY)
    TP = max(T, 128)
    dma = pltpu.SemaphoreType.DMA

    def each(chunks, *shape):
        return [pltpu.VMEM((*shape, w), BF16) for _, w in chunks]

    na, nb = len(A), len(B)
    scratch = [
        pltpu.VMEM((T, DZ), BF16),
        pltpu.VMEM((DZ,), BF16),
        pltpu.VMEM(expert_ids.shape[::-1], jnp.int32),
        pltpu.VMEM(expert_ids.shape[::-1], BF16),
        pltpu.VMEM((T, DZ), BF16),
        pltpu.VMEM((E, 1, 128), F32),
        pltpu.VMEM((E, 1, 128), F32),
        pltpu.VMEM((S, 128), F32),
        pltpu.VMEM((NZ * DZ, FFD), BF16),
        pltpu.VMEM((NZ * DZ, FFD), BF16),
        pltpu.VMEM((FFD, NZ * DZ), BF16),
        pltpu.VMEM((NZ, 8, TP), F32),
        pltpu.VMEM((S, T), BF16),
        pltpu.VMEM((T, S), BF16),
        pltpu.VMEM((S, FFD), F32),
        pltpu.VMEM((S, FFD), F32),
        pltpu.VMEM((S, FFD), BF16),
        dma((4,)),
        dma,
        dma((3,)),
        dma((10,)),
        dma((2,)),
        dma((1,)),
        [
            each(A, NZ, E, CAP),
            each(A, E, CAP),
            each(A, S),
            each(A, S),
            each(A, 2, S),
            each(A, 2, S),
            each(A, E, CAP),
            each(A, E, CAP),
        ],
        [
            each(B, E, NZ, CAP),
            each(B, NZ, T),
            each(B, E, NZ, CAP),
            each(B, E, NZ, CAP),
            each(B, E, NZ, CAP),
            each(B, T),
            each(B, T),
            each(B, 2, T),
            each(B, 2, T),
        ],
        [dma((na, 2)), dma((2, na, 2)), dma((2, na, 2)), dma((na,))],
        [dma((nb, 2)), dma((2, nb)), dma((2, nb)), dma((nb,))],
    ]
    return pl.pallas_call(
        functools.partial(moe_kernel, cfg),
        out_shape=jax.ShapeDtypeStruct((T, DZ), BF16),
        in_specs=[hbm] * 7,
        out_specs=hbm,
        scratch_shapes=scratch,
        compiler_params=pltpu.CompilerParams(
            collective_id=0, has_side_effects=True, vmem_limit_bytes=cfg["VMEM"]
        ),
        name="moe_layer",
    )(tokens, norm_gain, expert_ids.T, gate_prob.T, w_gate[0], w_up[0], w_down[0])


def config(mesh, tokens=8192, width=D, ff=2048, a=WIDTHS_A, b=WIDTHS_B, nx=4):
    E = mesh.shape["ep"]
    DZ = width // NZ
    chunks, lo = [], 0
    for w in (*a, *b):
        chunks.append((lo, w))
        lo += w
    assert lo == DZ
    return dict(
        E=E,
        T=tokens // E,
        D=width,
        DZ=DZ,
        FFD=ff // NZ,
        A=chunks[: len(a)],
        B=chunks[len(a) :],
        NX=nx,
        STRIDE=11,
        VMEM=67_000_000,
    )


def build(mesh, cfg):
    placed = (
        P("ep", "tp"),
        P("tp"),
        P("ep", None),
        P("ep", None),
        P("ep", None, "tp"),
        P("ep", None, "tp"),
        P("ep", "tp", None),
    )
    return jax.shard_map(
        functools.partial(local, cfg), mesh=mesh, in_specs=placed, out_specs=P("ep", "tp"), check_vma=False
    )


def solution(mesh):
    return build(mesh, config(mesh))
```

```python
import functools

import jax
import jax.numpy as jnp
from jax import lax
from jax.experimental import pallas as pl
from jax.experimental.pallas import tpu as pltpu
from jax.sharding import PartitionSpec as P

MESH = pl.DeviceIdType.MESH
F32 = jnp.float32
BF16 = jnp.bfloat16

D = 7168
CAP = 16
CORES = 2
NZ = 4
WIDTHS_A = (256, 256, 256, 256)
WIDTHS_B = (256, 256, 256)
WEIGHT_PIECES = 4
epsilon = 1e-06


def moe_kernel(
    cfg,
    tokens_hbm,
    gain_hbm,
    ids_hbm,
    prob_hbm,
    wg_hbm,
    wu_hbm,
    wd_hbm,
    out_hbm,
    tokens,
    gain_ref,
    ids_ref,
    prob_ref,
    out_v,
    sc_out,
    sc_in,
    scales,
    wg,
    wu,
    wd,
    sq_buf,
    disp_t,
    comb,
    acc_g,
    acc_u,
    hid,
    t_sem,
    o_sem,
    w_sem,
    sent,
    sc_recv,
    sq_recv,
    per_a,
    per_b,
    sem_a,
    sem_b,
):
    xa, out_a, far_a, far_in_a, near_a, near_in_a, back_a, ret_a = per_a
    xb, nb, out_b, back_b, ret_b, far_b, far_in_b, near_b, near_in_b = per_b
    da_recv, za_recv, ra_recv, ya_recv = sem_a
    db_recv, zb_recv, rb_recv, yb_recv = sem_b
    da_send, db_send, za_send, zb_send, ra_send, rb_send, ya_send, yb_send, sc_send, sq_send = (
        sent.at[i] for i in range(10)
    )
    E, A, B = cfg["E"], cfg["A"], cfg["B"]
    NA, NB = len(A), len(B)
    DZ, T = cfg["DZ"], cfg["T"]
    S = E * CAP
    EH, EQ = E // 2, E // 4
    SH, SQ = S // 2, S // 4
    TH = T // 2
    e = lax.axis_index("ep")
    z = lax.axis_index("tp")
    zp = lax.rem(z + 1, NZ)
    zm = lax.rem(z + 3, NZ)
    zf = lax.rem(z + 2, NZ)

    def moved(off, sign):
        off = jnp.int32(off)
        nx, ny = cfg["NX"], E // CORES // cfg["NX"]
        mine, step = e // CORES, off // CORES
        py = lax.rem(mine // nx + sign * (step // nx) + ny, ny)
        px = lax.rem(lax.rem(mine, nx) + sign * lax.rem(step, nx) + nx, nx)
        core = lax.rem(lax.rem(e, CORES) + sign * lax.rem(off, CORES) + CORES, CORES)
        return (py * nx + px) * CORES + core

    def peer_of(k):
        return moved(lax.rem(k * cfg["STRIDE"], E), 1)

    def origin_of(k):
        return moved(lax.rem(k * cfg["STRIDE"], E), -1)

    def to_z(src, dst, send, recv, zt):
        return pltpu.make_async_remote_copy(
            src_ref=src, dst_ref=dst, send_sem=send, recv_sem=recv, device_id=(e, zt), device_id_type=MESH
        )

    def to_e(src, dst, send, recv, et):
        return pltpu.make_async_remote_copy(
            src_ref=src, dst_ref=dst, send_sem=send, recv_sem=recv, device_id=(et, z), device_id_type=MESH
        )

    def take(ref, sem):
        pltpu.make_async_copy(ref, ref, sem).wait()

    small_copies = [
        pltpu.make_async_copy(src, dst, t_sem.at[n])
        for n, (src, dst) in enumerate(
            ((ids_hbm, ids_ref), (prob_hbm, prob_ref), (gain_hbm, gain_ref), (tokens_hbm, tokens))
        )
    ]
    for copy in small_copies:
        copy.start()
    barrier = pltpu.get_barrier_semaphore()

    def hops(k):
        step, nx, ny = k // CORES, cfg["NX"], E // CORES // cfg["NX"]
        dx, dy = step % nx, step // nx
        return min(dx, nx - dx) + min(dy, ny - dy)

    for k in sorted(range(1, E), key=hops, reverse=True):
        pl.semaphore_signal(barrier, inc=1, device_id=(moved(k, 1), z), device_id_type=MESH)
    for dz in (2, 1, 3):
        pl.semaphore_signal(barrier, inc=1, device_id=(e, lax.rem(z + dz, NZ)), device_id_type=MESH)
    for copy in small_copies[:3]:
        copy.wait()

    rows_w = wg.shape[0] // WEIGHT_PIECES
    rows_d = wd.shape[0] // WEIGHT_PIECES
    weight_copies = []
    for p in range(WEIGHT_PIECES):
        rs = pl.ds(p * rows_w, rows_w)
        weight_copies.append(pltpu.make_async_copy(wg_hbm.at[rs], wg.at[rs], w_sem.at[0]))
        weight_copies.append(pltpu.make_async_copy(wu_hbm.at[rs], wu.at[rs], w_sem.at[1]))
    down_copies = []
    for p in range(WEIGHT_PIECES):
        rs = pl.ds(p * rows_d, rows_d)
        down_copies.append(pltpu.make_async_copy(wd_hbm.at[rs], wd.at[rs], w_sem.at[2]))

    ids = ids_ref[...]
    probs = prob_ref[...].astype(F32)
    expert_iota = lax.broadcasted_iota(jnp.int32, (E, T), 0)
    match = jnp.zeros((E, T), F32)
    weight = jnp.zeros((E, T), F32)
    for k in range(ids.shape[0]):
        hit = ids[k : k + 1, :] == expert_iota
        match = match + jnp.where(hit, 1.0, 0.0)
        weight = weight + jnp.where(hit, probs[k : k + 1, :], 0.0)
    earlier = jnp.where(
        lax.broadcasted_iota(jnp.int32, (T, T), 0) < lax.broadcasted_iota(jnp.int32, (T, T), 1), 1.0, 0.0
    ).astype(BF16)
    match_b = match.astype(BF16)
    before = jnp.dot(match_b, earlier, preferred_element_type=F32).astype(BF16)
    spread = jnp.where(
        lax.broadcasted_iota(jnp.int32, (S, E), 0) // CAP == lax.broadcasted_iota(jnp.int32, (S, E), 1), 1.0, 0.0
    )
    spread_b = spread.astype(BF16)
    match_s = jnp.dot(spread_b, match_b, preferred_element_type=F32)
    before_s = jnp.dot(spread_b, before, preferred_element_type=F32)
    weight_s = jnp.dot(spread_b, weight.astype(BF16), preferred_element_type=F32)
    slot_of = lax.rem(lax.broadcasted_iota(jnp.int32, (S, T), 0), CAP).astype(F32)
    chosen = jnp.where((match_s > 0.5) & (before_s == slot_of), 1.0, 0.0)
    disp_t[...] = chosen.astype(BF16)
    small_copies[3].wait()
    for copy in weight_copies + down_copies:
        copy.start()

    def scaled(at):
        lo, w = at
        gain = gain_ref[pl.ds(lo, w)].astype(F32).reshape(1, w)
        return (tokens[:, pl.ds(lo, w)].astype(F32) * gain).astype(BF16)

    def to_experts(src, dst, send, recv, h):
        def one(k, carry):
            et = peer_of(k)
            to_e(src.at[et], dst.at[k], send, recv, et).start()
            return carry

        lax.fori_loop(max(1, h * EH), (h + 1) * EH, one, 0)

    def to_origins(src, dst, send, recv, h):
        def one(k, carry):
            to_e(src.at[k], dst.at[e], send, recv, origin_of(k)).start()
            return carry

        lax.fori_loop(max(1, h * EH), (h + 1) * EH, one, 0)

    def half(h):
        return pl.ds(h * EH, EH)

    rest = pl.ds(0, E - 1)

    def others(h):
        return pl.ds(0, EH - 1 if h == 0 else EH)

    def scale_b(c):
        nb[c][z] = scaled(B[c])

    def direct_b(c):
        for i, zt in ((0, zp), (1, zm)):
            to_z(nb[c].at[z], nb[c].at[z], zb_send, zb_recv.at[0, c], zt).start()

    def fill_a(c):
        rows = jnp.dot(disp_t[...], scaled(A[c]), preferred_element_type=F32).astype(BF16)
        out_a[c][...] = rows.reshape(E, CAP, A[c][1])

    def dispatch_a(c, h):
        if h == 0 and c > 1:
            fill_a(c)
        to_experts(out_a[c], xa[c].at[z], da_send, da_recv.at[c, h], h)
        if h == 0:
            xa[c][z, 0] = out_a[c][e]

    def squares():
        TP = max(T, 128)
        values = tokens[...].astype(F32)
        part = jnp.sum(values * values, axis=1, keepdims=True)
        if T < 128:
            part = jnp.concatenate([part, jnp.zeros((128 - T, 1), F32)], axis=0)
        part_t = jnp.transpose(jnp.broadcast_to(part, (TP, 128)))
        sq_buf[z] = part_t[0:8, :]
        for copy in sq_copies:
            copy.start()

    sq_copies = [
        to_z(sq_buf.at[z], sq_buf.at[z], sq_send, sq_recv.at[0], lax.rem(z + dz, NZ))
        for dz in range(1, NZ)
    ]

    def prepare():
        comb[...] = jnp.transpose(chosen * weight_s).astype(BF16)
        acc_g[...] = jnp.zeros_like(acc_g)
        acc_u[...] = jnp.zeros_like(acc_u)

    def lane_of_slot():
        lane = lax.broadcasted_iota(jnp.int32, (S, 128), 1)
        return lane == lax.rem(lax.broadcasted_iota(jnp.int32, (S, 128), 0), CAP)

    def send_scales():
        take(sq_buf.at[pl.ds(0, NZ - 1)], sq_recv.at[0])
        total = (sq_buf[0] + sq_buf[1] + sq_buf[2] + sq_buf[3])[0:1, 0:T]
        inverse = lax.rsqrt(total / cfg["D"] + epsilon)
        per_slot = jnp.sum(disp_t[...].astype(F32) * inverse, axis=1, keepdims=True)
        laned = jnp.where(lane_of_slot(), per_slot, 0.0)
        owner = jnp.where(
            lax.broadcasted_iota(jnp.int32, (E, S), 1) // CAP == lax.broadcasted_iota(jnp.int32, (E, S), 0), 1.0, 0.0
        )
        table = jnp.dot(owner, laned, preferred_element_type=F32, precision=lax.Precision.HIGHEST)
        sc_out[...] = table.reshape(E, 1, 128)
        for h in range(2):
            to_experts(sc_out, sc_in, sc_send, sc_recv.at[h], h)
        sc_in[0] = sc_out[e]

    def take_scales():
        for h in range(2):
            take(sc_in.at[others(h)], sc_recv.at[h])
        owner = jnp.where(
            lax.broadcasted_iota(jnp.int32, (S, E), 0) // CAP == lax.broadcasted_iota(jnp.int32, (S, E), 1), 1.0, 0.0
        )
        rows = jnp.dot(
            owner, sc_in[...].reshape(E, 128), preferred_element_type=F32, precision=lax.Precision.HIGHEST
        )
        per_row = jnp.sum(jnp.where(lane_of_slot(), rows, 0.0), axis=1, keepdims=True)
        scales[...] = jnp.broadcast_to(per_row, (S, 128))

    def forward_b(c):
        lo, hi = pl.ds(0, TH), pl.ds(TH, TH)
        take(nb[c].at[pl.ds(0, 2)], zb_recv.at[0, c])
        to_z(nb[c].at[zm, lo], nb[c].at[zm, lo], zb_send, zb_recv.at[1, c], zp).start()
        to_z(nb[c].at[zp, hi], nb[c].at[zp, hi], zb_send, zb_recv.at[1, c], zm).start()

    def dispatch_b(c, h):
        if h == 0:
            take(nb[c].at[zf], zb_recv.at[1, c])
            for q in range(NZ):
                rows = jnp.dot(disp_t[...], nb[c][q], preferred_element_type=F32).astype(BF16)
                out_b[c][:, q] = rows.reshape(E, CAP, B[c][1])
        to_experts(out_b[c], xb[c], db_send, db_recv.at[c, h], h)
        if h == 0:
            xb[c][0] = out_b[c][e]

    def direct_a(c, h):
        take(xa[c].at[z, others(h)], da_recv.at[c, h])
        rows = xa[c].at[z, half(h)]
        for i, zt in ((0, zp), (1, zm)):
            to_z(rows, rows, za_send, za_recv.at[0, c, h], zt).start()

    def forward_a(c, h):
        take(xa[c].at[pl.ds(0, 2), half(h)], za_recv.at[0, c, h])
        rows = xa[c].at[zm, pl.ds(h * EH, EQ)]
        to_z(rows, rows, za_send, za_recv.at[1, c, h], zp).start()
        rows = xa[c].at[zp, pl.ds(h * EH + EQ, EQ)]
        to_z(rows, rows, za_send, za_recv.at[1, c, h], zm).start()

    def multiply(blocks, at, h):
        base, width = at
        x = jnp.concatenate([b.reshape(SH, width) for b, _ in blocks], axis=1)
        for w_ref, acc in ((wg, acc_g), (wu, acc_u)):
            w = jnp.concatenate(
                [w_ref[pl.ds(pl.multiple_of(q * DZ + base, 128), width), :] for _, q in blocks], axis=0
            )
            acc[half_rows(h)] += jnp.dot(x, w, preferred_element_type=F32)

    def half_rows(h):
        return pl.ds(h * SH, SH)

    def multiply_near(c, h):
        multiply([(xa[c][q, half(h)], q) for q in (z, zp, zm)], A[c], h)

    def multiply_far(c, h):
        take(xa[c].at[zf, half(h)], za_recv.at[1, c, h])
        multiply([(xa[c][zf, half(h)], zf)], A[c], h)

    def multiply_b(c, h):
        take(xb[c].at[others(h)], db_recv.at[c, h])
        multiply([(xb[c][half(h), q], q) for q in range(NZ)], B[c], h)

    def wait_weights():
        take(wg, w_sem.at[0])
        take(wu, w_sem.at[1])

    def enter():
        pl.semaphore_wait(barrier, E - 1 + NZ - 1)

    def hidden(h):
        rows = half_rows(h)
        scale = scales[rows, 0:1]
        g = acc_g[rows] * scale
        hid[rows] = (g / (1.0 + jnp.exp(-g)) * (acc_u[rows] * scale)).astype(BF16)

    def wait_down():
        take(wd, w_sem.at[2])

    def down(q, at, h):
        lo, w = at
        ds = pl.ds(pl.multiple_of(q * DZ + lo, 128), w)
        return jnp.dot(hid[half_rows(h)], wd[:, ds], preferred_element_type=F32).astype(BF16)

    lo_t, hi_t = pl.ds(0, TH), pl.ds(TH, TH)

    def plus(a, b):
        return (a.astype(F32) + b.astype(F32)).astype(BF16)

    def quarters(h):
        return pl.ds(h * SH, SQ), pl.ds(h * SH + SQ, SQ)

    def far_part_a(c, h):
        lo, hi = quarters(h)
        far_a[c][half_rows(h)] = down(zf, A[c], h)
        to_z(far_a[c].at[lo], far_in_a[c].at[lo], ra_send, ra_recv.at[0, c, h], zp).start()
        to_z(far_a[c].at[hi], far_in_a[c].at[hi], ra_send, ra_recv.at[0, c, h], zm).start()

    def near_part_a(c, h):
        lo, hi = quarters(h)
        rows = half_rows(h)
        near_a[c][0, rows] = down(zp, A[c], h)
        near_a[c][1, rows] = down(zm, A[c], h)
        take(far_in_a[c].at[rows], ra_recv.at[0, c, h])
        near_a[c][0, lo] = plus(near_a[c][0, lo], far_in_a[c][lo])
        to_z(near_a[c].at[0, rows], near_in_a[c].at[0, rows], ra_send, ra_recv.at[1, c, h], zp).start()
        near_a[c][1, hi] = plus(near_a[c][1, hi], far_in_a[c][hi])
        to_z(near_a[c].at[1, rows], near_in_a[c].at[1, rows], ra_send, ra_recv.at[1, c, h], zm).start()

    def own_part_a(c, h):
        rows = half_rows(h)
        own = down(z, A[c], h).astype(F32)
        take(near_in_a[c].at[:, rows], ra_recv.at[1, c, h])
        own = own + near_in_a[c][0, rows].astype(F32) + near_in_a[c][1, rows].astype(F32)
        back_a[c][half(h)] = own.astype(BF16).reshape(EH, CAP, A[c][1])
        to_origins(back_a[c], ret_a[c], ya_send, ya_recv.at[c], h)
        if h == 0:
            ret_a[c][e] = back_a[c][0]

    def part_b(c, h):
        for q in range(NZ):
            back_b[c][half(h), q] = down(q, B[c], h).reshape(EH, CAP, B[c][1])
        to_origins(back_b[c], ret_b[c], yb_send, yb_recv.at[c], h)
        if h == 0:
            ret_b[c][e] = back_b[c][0]

    def weigh_b(c, q):
        return jnp.dot(comb[...], ret_b[c][:, q].reshape(S, B[c][1]), preferred_element_type=F32)

    def far_part_b(c):
        take(ret_b[c].at[rest], yb_recv.at[c])
        far_b[c][...] = weigh_b(c, zf).astype(BF16)
        to_z(far_b[c].at[lo_t], far_in_b[c].at[lo_t], rb_send, rb_recv.at[0, c], zp).start()
        to_z(far_b[c].at[hi_t], far_in_b[c].at[hi_t], rb_send, rb_recv.at[0, c], zm).start()

    def near_part_b(c):
        near_b[c][0] = weigh_b(c, zp).astype(BF16)
        near_b[c][1] = weigh_b(c, zm).astype(BF16)
        take(far_in_b[c], rb_recv.at[0, c])
        near_b[c][0, lo_t] = plus(near_b[c][0, lo_t], far_in_b[c][lo_t])
        to_z(near_b[c].at[0], near_in_b[c].at[0], rb_send, rb_recv.at[1, c], zp).start()
        near_b[c][1, hi_t] = plus(near_b[c][1, hi_t], far_in_b[c][hi_t])
        to_z(near_b[c].at[1], near_in_b[c].at[1], rb_send, rb_recv.at[1, c], zm).start()

    def own_part_b(c):
        own = weigh_b(c, z)
        take(near_in_b[c], rb_recv.at[1, c])
        own = own + near_in_b[c][0].astype(F32) + near_in_b[c][1].astype(F32)
        out_v[:, pl.ds(*B[c])] = own.astype(BF16)
        write_out(NA + c).start()

    def write_out(n):
        at = pl.ds(*(A + B)[n])
        return pltpu.make_async_copy(out_v.at[:, at], out_hbm.at[:, at], o_sem)

    def combine_a(c):
        take(ret_a[c].at[rest], ya_recv.at[c])
        got = jnp.dot(comb[...], ret_a[c][...].reshape(S, A[c][1]), preferred_element_type=F32)
        out_v[:, pl.ds(*A[c])] = got.astype(BF16)
        write_out(c).start()

    order = (
        (scale_b, 0), (scale_b, 1), (scale_b, 2), (fill_a, 0), (fill_a, 1), (enter,), (direct_b, 0), (dispatch_a, 0, 0), (direct_b, 1),
        (dispatch_a, 0, 1), (direct_b, 2), (dispatch_a, 1, 0), (dispatch_a, 1, 1), (squares,), (dispatch_a, 2, 0),
        (dispatch_a, 2, 1), (forward_b, 0), (dispatch_a, 3, 0), (dispatch_a, 3, 1), (prepare,), (forward_b, 1),
        (direct_a, 0, 0), (direct_a, 0, 1), (forward_b, 2), (send_scales,), (dispatch_b, 0, 0), (dispatch_b, 0, 1),
        (direct_a, 1, 0), (direct_a, 1, 1), (dispatch_b, 1, 0), (dispatch_b, 1, 1), (wait_weights,),
        (forward_a, 0, 0), (direct_a, 2, 0), (forward_a, 0, 1), (direct_a, 2, 1), (dispatch_b, 2, 0),
        (dispatch_b, 2, 1), (multiply_near, 0, 0), (multiply_near, 0, 1), (forward_a, 1, 0), (direct_a, 3, 0),
        (forward_a, 1, 1), (direct_a, 3, 1), (multiply_far, 0, 0), (multiply_far, 0, 1), (multiply_near, 1, 0),
        (multiply_near, 1, 1), (take_scales,), (multiply_b, 0, 0), (multiply_far, 1, 0), (multiply_b, 0, 1),
        (forward_a, 2, 0), (multiply_far, 1, 1), (multiply_near, 2, 0), (forward_a, 2, 1), (multiply_near, 2, 1),
        (forward_a, 3, 0), (multiply_b, 1, 0), (multiply_far, 2, 0), (multiply_b, 1, 1), (multiply_near, 3, 0),
        (multiply_far, 2, 1), (wait_down,), (forward_a, 3, 1), (multiply_b, 2, 0), (multiply_near, 3, 1),
        (multiply_far, 3, 0), (hidden, 0), (part_b, 1, 0), (far_part_a, 0, 0), (part_b, 0, 0), (far_part_a, 1, 0),
        (multiply_far, 3, 1), (multiply_b, 2, 1), (hidden, 1), (far_part_a, 0, 1), (part_b, 0, 1),
        (near_part_a, 0, 0), (far_part_a, 1, 1), (part_b, 1, 1), (near_part_a, 0, 1), (far_part_a, 2, 0),
        (near_part_a, 1, 0), (part_b, 2, 0), (far_part_a, 2, 1), (part_b, 2, 1), (near_part_a, 1, 1),
        (own_part_a, 0, 0), (far_part_a, 3, 0), (near_part_a, 2, 0), (own_part_a, 0, 1), (far_part_b, 0),
        (far_part_a, 3, 1), (near_part_a, 2, 1), (own_part_a, 1, 0), (own_part_a, 1, 1), (near_part_b, 0),
        (near_part_a, 3, 0), (own_part_a, 2, 0), (far_part_b, 1), (near_part_a, 3, 1), (own_part_a, 2, 1),
        (own_part_a, 3, 0), (far_part_b, 2), (near_part_b, 1), (own_part_a, 3, 1), (near_part_b, 2), (combine_a, 0),
        (own_part_b, 0), (combine_a, 1), (own_part_b, 1), (combine_a, 2), (own_part_b, 2), (combine_a, 3),
    )
    for step, *at in order:
        step(*at)

    take(out_v, o_sem)
    wa, wb = (sum(w for _, w in chunks) for chunks in (A, B))
    for sem, count in (
        (da_send, (S - CAP) * wa),
        (db_send, (S - CAP) * NZ * wb),
        (za_send, 3 * S * wa),
        (zb_send, 3 * T * wb),
        (ra_send, 3 * S * wa),
        (rb_send, 3 * T * wb),
        (ya_send, (S - CAP) * wa),
        (yb_send, (S - CAP) * NZ * wb),
    ):
        take(wg.at[pl.ds(0, count // wg.shape[1])], sem)
    take(sc_out.at[rest], sc_send)
    take(sq_buf.at[pl.ds(0, NZ - 1)], sq_send)


def local(cfg, tokens, norm_gain, expert_ids, gate_prob, w_gate, w_up, w_down):
    E, T, A, B = cfg["E"], cfg["T"], cfg["A"], cfg["B"]
    DZ, FFD = cfg["DZ"], cfg["FFD"]
    S = E * CAP
    hbm = pl.BlockSpec(memory_space=pl.ANY)
    TP = max(T, 128)
    dma = pltpu.SemaphoreType.DMA

    def each(chunks, *shape):
        return [pltpu.VMEM((*shape, w), BF16) for _, w in chunks]

    na, nb = len(A), len(B)
    scratch = [
        pltpu.VMEM((T, DZ), BF16),
        pltpu.VMEM((DZ,), BF16),
        pltpu.VMEM(expert_ids.shape[::-1], jnp.int32),
        pltpu.VMEM(expert_ids.shape[::-1], BF16),
        pltpu.VMEM((T, DZ), BF16),
        pltpu.VMEM((E, 1, 128), F32),
        pltpu.VMEM((E, 1, 128), F32),
        pltpu.VMEM((S, 128), F32),
        pltpu.VMEM((NZ * DZ, FFD), BF16),
        pltpu.VMEM((NZ * DZ, FFD), BF16),
        pltpu.VMEM((FFD, NZ * DZ), BF16),
        pltpu.VMEM((NZ, 8, TP), F32),
        pltpu.VMEM((S, T), BF16),
        pltpu.VMEM((T, S), BF16),
        pltpu.VMEM((S, FFD), F32),
        pltpu.VMEM((S, FFD), F32),
        pltpu.VMEM((S, FFD), BF16),
        dma((4,)),
        dma,
        dma((3,)),
        dma((10,)),
        dma((2,)),
        dma((1,)),
        [
            each(A, NZ, E, CAP),
            each(A, E, CAP),
            each(A, S),
            each(A, S),
            each(A, 2, S),
            each(A, 2, S),
            each(A, E, CAP),
            each(A, E, CAP),
        ],
        [
            each(B, E, NZ, CAP),
            each(B, NZ, T),
            each(B, E, NZ, CAP),
            each(B, E, NZ, CAP),
            each(B, E, NZ, CAP),
            each(B, T),
            each(B, T),
            each(B, 2, T),
            each(B, 2, T),
        ],
        [dma((na, 2)), dma((2, na, 2)), dma((2, na, 2)), dma((na,))],
        [dma((nb, 2)), dma((2, nb)), dma((2, nb)), dma((nb,))],
    ]
    return pl.pallas_call(
        functools.partial(moe_kernel, cfg),
        out_shape=jax.ShapeDtypeStruct((T, DZ), BF16),
        in_specs=[hbm] * 7,
        out_specs=hbm,
        scratch_shapes=scratch,
        compiler_params=pltpu.CompilerParams(
            collective_id=0, has_side_effects=True, vmem_limit_bytes=cfg["VMEM"]
        ),
        name="moe_layer",
    )(tokens, norm_gain, expert_ids.T, gate_prob.T, w_gate[0], w_up[0], w_down[0])


def config(mesh, tokens=8192, width=D, ff=2048, a=WIDTHS_A, b=WIDTHS_B, nx=4):
    E = mesh.shape["ep"]
    DZ = width // NZ
    chunks, lo = [], 0
    for w in (*a, *b):
        chunks.append((lo, w))
        lo += w
    assert lo == DZ
    return dict(
        E=E,
        T=tokens // E,
        D=width,
        DZ=DZ,
        FFD=ff // NZ,
        A=chunks[: len(a)],
        B=chunks[len(a) :],
        NX=nx,
        STRIDE=11,
        VMEM=67_000_000,
    )


def build(mesh, cfg):
    placed = (
        P("ep", "tp"),
        P("tp"),
        P("ep", None),
        P("ep", None),
        P("ep", None, "tp"),
        P("ep", None, "tp"),
        P("ep", "tp", None),
    )
    return jax.shard_map(
        functools.partial(local, cfg), mesh=mesh, in_specs=placed, out_specs=P("ep", "tp"), check_vma=False
    )


def solution(mesh):
    return build(mesh, config(mesh))
```
